256 devices in a mesh: dp: 32 (over z, y_hi, core), tensor: 8 (over x, y_lo).
Axes of the slice: x: 4, y: 4 (y_hi: 2, y_lo: 2; y = y_hi * 2 + y_lo), z: 8, core: 2. Of those that a mesh axis runs over, the one named last changes fastest.
Arguments:
- tokens: bfloat16 [128, 576, 1024], P('dp', 'tensor'), may hold values from -150 to 150
- cotangent: bfloat16 [128, 576, 1024], P('dp', 'tensor'), may hold values from -6 to 6
- dispatch_weight: bfloat16 [1024, 64], replicated, may hold values from -3 to 3
- w_in: bfloat16 [64, 1024, 4096], P('dp', None, 'tensor'), may hold values from -0.1875 to 0.1875
- w_out: bfloat16 [64, 4096, 1024], P('dp', 'tensor'), may hold values from -0.09375 to 0.09375
Outputs:
- grad_tokens: bfloat16 [128, 576, 1024], P('dp', 'tensor')
- grad_router: float32 [1024, 64], replicated
- grad_w_in: bfloat16 [64, 1024, 4096], P('dp', None, 'tensor')
- grad_w_out: bfloat16 [64, 4096, 1024], P('dp', 'tensor')
The draws below stay inside these ranges and needn't reach their ends.
All inputs are finite; a program needn't handle non-finite values.
Results may differ from the reference program's by a relative error of at most 0.0079.
Values may be sent and summed in bfloat16 or wider, within the bound.
A program may use at most 64 MiB of HBM per device.

```python
import math
import jax
import jax.numpy as jnp
from jax import lax

D = 1024
FF = 4096
EXPERTS = 64
IMAGES = 128
SEQ = 576


def drawn_pair(key):
    router_key = jax.random.fold_in(key, 101)
    token_key = jax.random.fold_in(key, 102)
    router = jnp.clip(jax.random.normal(router_key, (D, EXPERTS), jnp.float32), -6.0, 6.0) * (3.0 / math.sqrt(D))
    base = jnp.clip(jax.random.normal(token_key, (IMAGES, SEQ, D), jnp.float32), -6.0, 6.0)
    position = jnp.arange(SEQ, dtype=jnp.float32) / max(SEQ - 1, 1)
    base = base * (0.6 * 3.0 ** position)[None, :, None]
    return (base, router)


def draw_tokens(key, part):
    return drawn_pair(key)[0].astype(jnp.bfloat16)


def draw_dispatch_weight(key, part):
    return drawn_pair(key)[1].astype(jnp.bfloat16)


def block_levels(own_key, dims, cuts, smallest, largest):
    gain = 1.0
    for axis_at, shards_of in cuts:
        draws = jax.random.uniform(jax.random.fold_in(jax.random.fold_in(own_key, 6), axis_at), (shards_of,), jnp.float32, smallest / len(cuts), largest / len(cuts))
        gain = gain * jnp.repeat(jnp.exp(draws), dims[axis_at] // shards_of).reshape((-1,) + (1,) * (len(dims) - 1 - axis_at))
    return gain


def bell_draw(own_key, dims, width, reach, split=(), kind=jnp.bfloat16):
    entries = jax.random.normal(own_key, dims, jnp.float32) * width
    if len(split) > 0:
        entries = block_levels(own_key, dims, split, -0.22, 0.18) * entries
    return jnp.clip(entries, min=-reach, max=reach).astype(kind)


def setup_inputs(seed: int = 0) -> dict:
    seeds = jax.random.split(jax.random.key(seed), 6)
    tokens = draw_tokens(jax.random.fold_in(seeds[5], 71), 0)
    cotangent = bell_draw(seeds[1], (IMAGES, SEQ, D), 1.0, 6.0, ((0, 32), (1, 8)))
    dispatch_weight = draw_dispatch_weight(jax.random.fold_in(seeds[5], 71), 0)
    w_in = bell_draw(seeds[3], (EXPERTS, D, FF), D ** -0.5, 0.1875, ((0, 32), (2, 8)))
    w_out = bell_draw(seeds[4], (EXPERTS, FF, D), FF ** -0.5, 0.09375, ((0, 32), (1, 8)))
    return dict(tokens=tokens, cotangent=cotangent, dispatch_weight=dispatch_weight, w_in=w_in, w_out=w_out)


def rounded(values):
    return lax.optimization_barrier(values.astype(jnp.bfloat16)).astype(jnp.float32)

def expert_forward(operands):
    slot_rows, first_mat, second_mat = operands
    pre_act = jnp.einsum('id,df->if', slot_rows, first_mat.astype(jnp.float32))
    hidden_low = rounded(jax.nn.gelu(pre_act))
    return jnp.einsum('if,fd->id', hidden_low, second_mat.astype(jnp.float32)).astype(jnp.bfloat16)

def expert_backward(operands):
    slot_rows, grad_rows, first_mat, second_mat = operands
    first_wide = first_mat.astype(jnp.float32)
    second_wide = second_mat.astype(jnp.float32)
    pre_act = jnp.einsum('id,df->if', slot_rows, first_wide)
    hidden_act, gelu_back = jax.vjp(jax.nn.gelu, pre_act)
    hidden_low = rounded(hidden_act)
    grad_hidden = jnp.einsum('id,fd->if', grad_rows, second_wide)
    grad_pre = rounded(gelu_back(grad_hidden)[0])
    grad_second = jnp.einsum('if,id->fd', hidden_low, grad_rows).astype(jnp.bfloat16)
    grad_first = jnp.einsum('id,if->df', slot_rows, grad_pre).astype(jnp.bfloat16)
    grad_slot = jnp.einsum('if,df->id', grad_pre, first_wide).astype(jnp.bfloat16)
    return (grad_first, grad_second, grad_slot)

def reference(tokens, cotangent, dispatch_weight, w_in, w_out):
    token_vals = tokens.astype(jnp.float32)
    grad_vals = cotangent.astype(jnp.float32)
    router = dispatch_weight.astype(jnp.float32)
    logits = jnp.einsum('isd,de->ise', token_vals, router)
    dispatch = jax.nn.softmax(logits, axis=1)
    combine = jax.nn.softmax(logits, axis=2)
    dispatch_low = rounded(dispatch)
    combine_low = rounded(combine)
    slot_inputs = rounded(jnp.einsum('ise,isd->ied', dispatch_low, token_vals))
    slot_major = jnp.transpose(slot_inputs, (1, 0, 2))
    slot_outputs = lax.map(expert_forward, (slot_major, w_in, w_out))
    slot_outputs = jnp.transpose(slot_outputs, (1, 0, 2)).astype(jnp.float32)
    grad_combine = jnp.einsum('isd,ied->ise', grad_vals, slot_outputs)
    grad_slots_out = rounded(jnp.einsum('ise,isd->ied', combine_low, grad_vals))
    grad_major = jnp.transpose(grad_slots_out, (1, 0, 2))
    grad_w_in, grad_w_out, grad_slots_in = lax.map(expert_backward, (slot_major, grad_major, w_in, w_out))
    grad_slots_in = jnp.transpose(grad_slots_in, (1, 0, 2)).astype(jnp.float32)
    grad_dispatch = jnp.einsum('isd,ied->ise', token_vals, grad_slots_in)
    row_dot = lax.optimization_barrier(jnp.sum(grad_combine * combine, axis=2, keepdims=True))
    column_dot = lax.optimization_barrier(jnp.sum(grad_dispatch * dispatch, axis=1, keepdims=True))
    grad_logits = rounded(combine * (grad_combine - row_dot) + dispatch * (grad_dispatch - column_dot))
    grad_tokens = (jnp.einsum('ise,ied->isd', dispatch_low, grad_slots_in) + jnp.einsum('ise,de->isd', grad_logits, router)).astype(jnp.bfloat16)
    grad_router = jnp.einsum('isd,ise->de', token_vals, grad_logits)
    return (grad_tokens, grad_router, grad_w_in, grad_w_out)
```

```python
import jax
import jax.numpy as jnp
from jax import lax
from jax.sharding import PartitionSpec as P

WIDE = jnp.float32
LOW = jnp.bfloat16


def swapped(blocks, axis):
    return lax.all_to_all(blocks, axis, split_axis=0, concat_axis=0, tiled=True)


def sent_to_all(x, axis):
    return swapped(jnp.broadcast_to(x[None], (lax.axis_size(axis), *x.shape)), axis)


def to_blocks(x, parts):
    return jnp.moveaxis(x.reshape(*x.shape[:-1], parts, x.shape[-1] // parts), -2, 0)


def on_device(tokens, cotangent, dispatch_weight, w_in, w_out):
    tp = lax.axis_size("tensor")
    dp = lax.axis_size("dp")
    images, _, width = tokens.shape
    slots = dispatch_weight.shape[1]
    own = w_in.shape[0]
    part = width // tp
    logits = jnp.einsum("isd,de->ise", tokens, dispatch_weight, preferred_element_type=WIDE)
    local_max = jnp.max(logits, axis=1)
    weight = jnp.exp(logits - local_max[:, None, :])
    weight_low = weight.astype(LOW)
    combine = jax.nn.softmax(logits, axis=2)
    combine_low = combine.astype(LOW)
    rows = jnp.stack([
        jnp.einsum("ise,isd->ied", weight_low, tokens, preferred_element_type=WIDE),
        jnp.einsum("ise,isd->ied", combine_low, cotangent, preferred_element_type=WIDE),
    ]).astype(LOW)
    stats = sent_to_all(
        jnp.stack([local_max, jnp.sum(weight, axis=1), jnp.sum(weight_low.astype(WIDE), axis=1)]),
        "tensor",
    )
    top = jnp.max(stats[:, 0], axis=0)
    shrink = jnp.exp(stats[:, 0] - top)
    total = jnp.sum(stats[:, 1] * shrink, axis=0)
    total_low = jnp.sum(stats[:, 2] * shrink, axis=0)
    pieces = swapped(to_blocks(rows, tp), "tensor").astype(WIDE)
    slot_slice = jnp.sum(pieces[:, 0] * (shrink / total_low)[..., None], axis=0)
    grad_slice = jnp.sum(pieces[:, 1], axis=0)
    both = jnp.stack([slot_slice, grad_slice]).astype(LOW)
    both = both.reshape(2, images, dp, own, part).transpose(2, 0, 3, 1, 4)
    arrived = sent_to_all(swapped(both, "dp"), "tensor")
    full = arrived.transpose(2, 3, 1, 4, 0, 5).reshape(2, own, dp * images, width)
    slot_inputs, grad_slots_out = full[0], full[1]

    pre_act = jnp.einsum("eid,edf->eif", slot_inputs, w_in, preferred_element_type=WIDE)
    hidden_act, gelu_back = jax.vjp(jax.nn.gelu, pre_act)
    hidden_low = hidden_act.astype(LOW)
    out_part = jnp.einsum("eif,efd->eid", hidden_low, w_out, preferred_element_type=WIDE)
    grad_hidden = jnp.einsum("eid,efd->eif", grad_slots_out, w_out, preferred_element_type=WIDE)
    grad_pre = gelu_back(grad_hidden)[0].astype(LOW)
    in_part = jnp.einsum("eif,edf->eid", grad_pre, w_in, preferred_element_type=WIDE)
    grad_w_out = jnp.einsum(
        "eif,eid->efd", hidden_low, grad_slots_out, preferred_element_type=WIDE
    ).astype(LOW)
    grad_w_in = jnp.einsum(
        "eid,eif->edf", slot_inputs, grad_pre, preferred_element_type=WIDE
    ).astype(LOW)

    back = jnp.stack([out_part, in_part]).astype(LOW)
    back = back.reshape(2, own, dp, images, tp, part).transpose(4, 2, 0, 1, 3, 5)
    summed = jnp.sum(swapped(back, "tensor").astype(WIDE), axis=0).astype(LOW)
    home = swapped(summed, "dp")
    in_slice = home[:, 1].transpose(2, 0, 1, 3).reshape(images, slots, part).astype(WIDE)
    column_dot = jnp.sum(sent_to_all(jnp.sum(in_slice * slot_slice, axis=2), "tensor"), axis=0)
    gathered = sent_to_all(home, "tensor")
    gathered = gathered.transpose(2, 4, 1, 3, 0, 5).reshape(2, images, slots, width)
    slot_outputs, grad_slots_in = gathered[0], gathered[1]

    dispatch = weight * (jnp.exp(local_max - top) / total)[:, None, :]
    dispatch_low = dispatch.astype(LOW)
    grad_combine = jnp.einsum("isd,ied->ise", cotangent, slot_outputs, preferred_element_type=WIDE)
    grad_dispatch = jnp.einsum("isd,ied->ise", tokens, grad_slots_in, preferred_element_type=WIDE)
    row_dot = jnp.sum(grad_combine * combine, axis=2, keepdims=True)
    grad_logits = (
        combine * (grad_combine - row_dot) + dispatch * (grad_dispatch - column_dot[:, None, :])
    ).astype(LOW)
    local_router = jnp.einsum("isd,ise->de", tokens, grad_logits, preferred_element_type=WIDE)
    token_part = jnp.einsum(
        "ise,ied->isd", dispatch_low, grad_slots_in, preferred_element_type=WIDE
    )
    router_part = jnp.einsum(
        "ise,de->isd", grad_logits, dispatch_weight, preferred_element_type=WIDE
    )
    grad_tokens = (token_part + router_part).astype(LOW)

    over_tensor = jnp.sum(swapped(local_router.reshape(tp, part, slots), "tensor"), axis=0)
    over_dp = jnp.sum(swapped(over_tensor.reshape(dp, part // dp, slots), "dp"), axis=0)
    router_slice = sent_to_all(over_dp, "dp").reshape(part, slots)
    grad_router = sent_to_all(router_slice, "tensor").reshape(width, slots)
    return (grad_tokens, grad_router, grad_w_in, grad_w_out)


def solution(mesh):
    return jax.shard_map(
        on_device,
        mesh=mesh,
        in_specs=(
            P("dp", "tensor", None),
            P("dp", "tensor", None),
            P(),
            P("dp", None, "tensor"),
            P("dp", "tensor", None),
        ),
        out_specs=(P("dp", "tensor", None), P(), P("dp", None, "tensor"), P("dp", "tensor", None)),
        check_vma=False,
    )
```

```python
import functools
import math

import jax
import jax.numpy as jnp
from jax import lax
from jax.experimental import pallas as pl
from jax.experimental.pallas import tpu as pltpu
from jax.sharding import PartitionSpec as P

WIDE = jnp.float32
LOW = jnp.bfloat16
MESH = pl.DeviceIdType.MESH
LANES = 128
LEAST = -3.0e38


def dot(a, b, over):
    return lax.dot_general(a, b, (over, ((), ())), preferred_element_type=WIDE)


def plain(a, b):
    return dot(a, b, ((1,), (0,)))


def rows_by_rows(a, b):
    return dot(a, b, ((1,), (1,)))


def columns_by_columns(a, b):
    return dot(a, b, ((0,), (0,)))


def iotas(shape):
    return lax.broadcasted_iota(jnp.int32, shape, 0), lax.broadcasted_iota(jnp.int32, shape, 1)


def kernel(
    tp, dp, images, own,
    tok, cot, router, w_in_hbm, w_out_hbm,
    grad_tok, grad_router, grad_in_hbm, grad_out_hbm,
    w_in, w_out, grad_in, grad_out, spread, weight, combine, dispatch, slot_slice,
    send_rows, recv_rows, send_slots, recv_slots, full, flat, sorted_rows, stats, stats_in,
    dots, dots_in, part, part_in, piece, piece_in, whole,
    local_sem, t_send, t_recv, d_send, d_recv,
):
    me_t, me_d = lax.axis_index("tensor"), lax.axis_index("dp")
    n = tok.shape[0]
    group = own * images
    c = dp * group
    seq = n // images
    slots = dp * own
    half = c // own

    def copy_tensor(phase, k, src, dst, slot):
        to = lax.rem(me_t + k, tp)
        return pltpu.make_async_remote_copy(
            src_ref=src(to), dst_ref=dst(slot),
            send_sem=t_send.at[phase, k], recv_sem=t_recv.at[phase, k],
            device_id={"tensor": to}, device_id_type=MESH,
        )

    def start_tensor(phase, src, dst):
        for k in range(1, tp):
            copy_tensor(phase, k, src, dst, me_t).start()

    def await_tensor(phase, src, dst):
        for k in range(1, tp):
            copy_tensor(phase, k, src, dst, lax.rem(me_t + tp - k, tp)).wait_recv()

    def drain_tensor(phase, src, dst):
        for k in range(1, tp):
            copy_tensor(phase, k, src, dst, me_t).wait_send()

    def start_dp(phase, src, dst):
        def one(k, carry):
            to = lax.rem(me_d + k, dp)
            pltpu.make_async_remote_copy(
                src_ref=src(to), dst_ref=dst(me_d),
                send_sem=d_send.at[phase], recv_sem=d_recv.at[phase],
                device_id={"dp": to}, device_id_type=MESH,
            ).start()
            return carry
        lax.fori_loop(1, dp, one, 0)

    def all_dp(phase, out, into):
        return pltpu.make_async_remote_copy(
            src_ref=out.at[pl.ds(0, dp - 1)], dst_ref=into.at[pl.ds(0, dp - 1)],
            send_sem=d_send.at[phase], recv_sem=d_recv.at[phase],
            device_id={"dp": lax.rem(me_d + 1, dp)}, device_id_type=MESH,
        )

    STATS, DOTS, PART, WHOLE = 8, 9, 10, 11
    rows_of = [
        (lot, lambda to, lot=lot: send_rows.at[lot, to], lambda s, lot=lot: recv_rows.at[lot, s])
        for lot in range(4)
    ]
    slots_of = [
        (4 + lot, lambda to, lot=lot: recv_slots.at[lot], lambda s, lot=lot: full.at[lot, s])
        for lot in range(4)
    ]
    stats_of = (STATS, lambda to: stats, lambda s: stats_in.at[s])
    dots_of = (DOTS, lambda to: dots, lambda s: dots_in.at[s])
    part_of = (PART, lambda to: part.at[to], lambda s: part_in.at[s])
    whole_of = (WHOLE, lambda to: whole.at[me_t], lambda s: whole.at[s])

    loads = [
        pltpu.make_async_copy(w_in_hbm, w_in, local_sem.at[0]),
        pltpu.make_async_copy(w_out_hbm, w_out, local_sem.at[1]),
    ]
    for load in loads:
        load.start()

    barrier = pltpu.get_barrier_semaphore()

    def greet(axis, me, size):
        def one(k, carry):
            pl.semaphore_signal(
                barrier, inc=1, device_id={axis: lax.rem(me + k, size)}, device_id_type=MESH
            )
            return carry
        lax.fori_loop(1, size, one, 0)

    greet("tensor", me_t, tp)
    greet("dp", me_d, dp)

    row, col = iotas((c, slots))
    choose = jnp.where((row >= col * images) & (row < col * images + images), 1.0, 0.0).astype(LOW)
    spread[...] = rows_by_rows(choose, router[...]).astype(LOW)
    row, col = iotas((c, n))
    begin = lax.rem(row, images) * seq
    ours = (col >= begin) & (col < begin + seq)
    masked = jnp.where(ours, rows_by_rows(spread[...], tok[...]), LEAST)
    top = jnp.max(masked, axis=1, keepdims=True)
    exponent = jnp.where(ours, jnp.exp(masked - top), 0.0)
    exponent_low = exponent.astype(LOW)
    weight[...] = exponent
    lane = iotas((c, LANES))[1]
    packed = jnp.where(
        lane == 0, top,
        jnp.where(
            lane == 1, jnp.sum(exponent, axis=1, keepdims=True),
            jnp.sum(exponent_low.astype(WIDE), axis=1, keepdims=True),
        ),
    )
    stats[...] = jnp.transpose(packed)[0:8, :]

    def cut(rows, lot):
        for t in range(tp):
            block = rows[:, t * LANES:(t + 1) * LANES].reshape(dp, group, LANES)
            send_rows[lot, t] = block.astype(LOW)

    cut(plain(exponent_low, tok[...]), 0)
    pl.semaphore_wait(barrier, tp + dp - 2)
    start_tensor(*stats_of)
    start_tensor(*rows_of[0])

    best = jnp.max(masked, axis=0, keepdims=True)
    raised = jnp.where(ours, jnp.exp(masked - best), 0.0)
    share = raised / jnp.sum(raised, axis=0, keepdims=True)
    combine[...] = share
    cut(plain(share.astype(LOW), cot[...]), 1)
    start_tensor(*rows_of[1])

    await_tensor(*stats_of)
    stats_in[me_t] = stats[...]
    most = stats_in[0, 0:1]
    for s in range(1, tp):
        most = jnp.maximum(most, stats_in[s, 0:1])
    shrinks = [jnp.exp(stats_in[s, 0:1] - most) for s in range(tp)]
    total = sum(stats_in[s, 1:2] * shrinks[s] for s in range(tp))
    total_low = sum(stats_in[s, 2:3] * shrinks[s] for s in range(tp))
    lines = [shrink / total_low for shrink in shrinks]
    lines.append(jnp.exp(stats[0:1] - most) / total)
    line_row = iotas((LANES, c))[0]
    table = jnp.zeros((LANES, c), WIDE)
    for s, line in enumerate(lines):
        table = jnp.where(line_row == s, line, table)
    table = jnp.transpose(table)
    dispatch[...] = weight[...] * table[:, tp:tp + 1]

    def summed(lot, scales=None):
        await_tensor(*rows_of[lot])
        recv_rows[lot, me_t] = send_rows[lot, me_t]
        total_rows = None
        for s in range(tp):
            term = recv_rows[lot, s].astype(WIDE).reshape(c, LANES)
            if scales is not None:
                term = term * scales[:, s:s + 1]
            total_rows = term if total_rows is None else total_rows + term
        return total_rows

    def pass_on(total_rows, lot):
        send_slots[lot] = total_rows.reshape(dp, group, LANES).astype(LOW)
        start_dp(lot, lambda to: send_slots.at[lot, to], lambda s: recv_slots.at[lot, s])

    def gather(lot):
        all_dp(lot, send_slots.at[lot], recv_slots.at[lot]).wait_recv()
        recv_slots[lot, me_d] = send_slots[lot, me_d]
        start_tensor(*slots_of[lot])

    def assembled(lot):
        await_tensor(*slots_of[lot])
        full[lot, me_t] = recv_slots[lot]
        for t in range(tp):
            block = full[lot, t].astype(WIDE).reshape(c, LANES)
            flat[lot, :, t * LANES:(t + 1) * LANES] = block.astype(LOW)
        return flat[lot]

    slot_slice[...] = summed(0, table)
    pass_on(slot_slice[...], 0)
    pass_on(summed(1), 1)
    gather(0)
    gather(1)

    def matching(q, other):
        late = (q >= half).astype(jnp.int32)
        image = lax.rem(q, images)
        return other == own * (q - late * half - image) + image + late * images

    row, col = iotas((c, c))
    sort = jnp.where(matching(row, col), 1.0, 0.0).astype(LOW)
    unsort = jnp.where(matching(col, row), 1.0, 0.0).astype(LOW)
    for load in loads:
        load.wait()
    root = math.sqrt(2.0 / math.pi)
    sorted_rows[0] = plain(sort, assembled(0)).astype(LOW)
    hidden, slope, results = [], [], []
    for e in range(own):
        pre = plain(sorted_rows[0, e * half:(e + 1) * half], w_in[e])
        square = pre * pre
        bent = jnp.tanh(root * (pre + 0.044715 * (square * pre)))
        hidden.append((0.5 * pre * (1.0 + bent)).astype(LOW))
        slope.append(
            0.5 * (1.0 + bent)
            + 0.5 * pre * (1.0 - bent * bent) * (root * (1.0 + 3.0 * 0.044715 * square))
        )
        results.append(plain(hidden[e], w_out[e]).astype(LOW))
    cut(plain(unsort, jnp.concatenate(results)), 2)
    start_tensor(*rows_of[2])
    sorted_rows[1] = plain(sort, assembled(1)).astype(LOW)
    grad_pre, results = [], []
    for e in range(own):
        grad_hidden = rows_by_rows(sorted_rows[1, e * half:(e + 1) * half], w_out[e])
        grad_pre.append((slope[e] * grad_hidden).astype(LOW))
        results.append(rows_by_rows(grad_pre[e], w_in[e]).astype(LOW))
    cut(plain(unsort, jnp.concatenate(results)), 3)
    start_tensor(*rows_of[3])
    for e in range(own):
        here = slice(e * half, (e + 1) * half)
        grad_out[e] = columns_by_columns(hidden[e], sorted_rows[1, here]).astype(LOW)
        grad_in[e] = columns_by_columns(sorted_rows[0, here], grad_pre[e]).astype(LOW)
    stores = [
        pltpu.make_async_copy(grad_in, grad_in_hbm, local_sem.at[2]),
        pltpu.make_async_copy(grad_out, grad_out_hbm, local_sem.at[3]),
    ]
    for store in stores:
        store.start()

    pass_on(summed(2), 2)
    pass_on(summed(3), 3)
    gather(2)
    gather(3)
    products = recv_slots[3].astype(WIDE).reshape(c, LANES) * slot_slice[...]
    own_dots = jnp.broadcast_to(jnp.sum(products, axis=1, keepdims=True), (c, LANES))
    dots[...] = jnp.transpose(own_dots)[0:8, :]
    start_tensor(*dots_of)

    slot_out = assembled(2)
    share = combine[...]
    grad_share = rows_by_rows(slot_out, cot[...])
    row_dot = jnp.sum(grad_share * share, axis=0, keepdims=True)
    from_share = share * (grad_share - row_dot)
    slot_grad = assembled(3)
    grad_weight = rows_by_rows(slot_grad, tok[...])
    await_tensor(*dots_of)
    dots_in[me_t] = dots[...]
    dot_line = dots_in[0, 0:1]
    for s in range(1, tp):
        dot_line = dot_line + dots_in[s, 0:1]
    column_dot = jnp.transpose(jnp.broadcast_to(dot_line, (LANES, c)))[:, 0:1]
    spots = dispatch[...]
    grad_logits = (from_share + spots * (grad_weight - column_dot)).astype(LOW)
    row, col = iotas((slots, c))
    fold = jnp.where((col >= row * images) & (col < row * images + images), 1.0, 0.0).astype(LOW)
    by_slot = plain(fold, grad_logits).astype(LOW)
    local_router = plain(by_slot, tok[...])
    for t in range(tp):
        part[t] = local_router[:, t * LANES:(t + 1) * LANES]
    start_tensor(*part_of)
    grad_tok[...] = (
        columns_by_columns(spots.astype(LOW), slot_grad)
        + columns_by_columns(grad_logits, spread[...])
    ).astype(LOW)

    await_tensor(*part_of)
    part_in[me_t] = part[me_t]
    router_rows = part_in[0]
    for s in range(1, tp):
        router_rows = router_rows + part_in[s]
    high = slots // dp
    for k in range(dp):
        piece[k] = router_rows[k * high:(k + 1) * high]
    start_dp(4, lambda to: piece.at[to], lambda s: piece_in.at[s])
    all_dp(4, piece, piece_in).wait_recv()
    piece_in[me_d] = piece[me_d]
    whole[me_t, me_d] = jnp.sum(piece_in[...], axis=0)
    start_dp(5, lambda to: whole.at[me_t, me_d], lambda s: whole.at[me_t, s])
    all_dp(5, whole.at[me_t], whole.at[me_t]).wait_recv()
    start_tensor(*whole_of)
    await_tensor(*whole_of)
    for t in range(tp):
        for k in range(dp):
            grad_router[k * high:(k + 1) * high, t * LANES:(t + 1) * LANES] = whole[t, k]

    for phase in [*rows_of, *slots_of, stats_of, dots_of, part_of, whole_of]:
        drain_tensor(*phase)
    for lot in range(4):
        all_dp(lot, send_slots.at[lot], recv_slots.at[lot]).wait_send()
    all_dp(4, piece, piece_in).wait_send()
    all_dp(5, whole.at[me_t], whole.at[me_t]).wait_send()
    for store in stores:
        store.wait()


def on_device(tokens, cotangent, dispatch_weight, w_in, w_out):
    tp, dp = lax.axis_size("tensor"), lax.axis_size("dp")
    images, seq, width = tokens.shape
    own, _, inner = w_in.shape
    n, slots, group = images * seq, dp * own, own * images
    c = dp * group
    vmem = pltpu.VMEM
    outs = pl.pallas_call(
        functools.partial(kernel, tp, dp, images, own),
        name="moe_back",
        out_shape=(
            jax.ShapeDtypeStruct((n, width), LOW),
            jax.ShapeDtypeStruct((slots, width), WIDE),
            jax.ShapeDtypeStruct(w_in.shape, LOW),
            jax.ShapeDtypeStruct(w_out.shape, LOW),
        ),
        in_specs=[pl.BlockSpec(memory_space=pltpu.VMEM)] * 3
        + [pl.BlockSpec(memory_space=pl.ANY)] * 2,
        out_specs=tuple(
            [pl.BlockSpec(memory_space=pltpu.VMEM)] * 2 + [pl.BlockSpec(memory_space=pl.ANY)] * 2
        ),
        scratch_shapes=[
            vmem(w_in.shape, LOW), vmem(w_out.shape, LOW),
            vmem(w_in.shape, LOW), vmem(w_out.shape, LOW),
            vmem((c, width), LOW),
            vmem((c, n), WIDE), vmem((c, n), WIDE), vmem((c, n), WIDE),
            vmem((c, LANES), WIDE),
            vmem((4, tp, dp, group, LANES), LOW), vmem((4, tp, dp, group, LANES), LOW),
            vmem((4, dp, group, LANES), LOW), vmem((4, dp, group, LANES), LOW),
            vmem((4, tp, dp, group, LANES), LOW),
            vmem((4, c, width), LOW), vmem((2, c, width), LOW),
            vmem((8, c), WIDE), vmem((tp, 8, c), WIDE),
            vmem((8, c), WIDE), vmem((tp, 8, c), WIDE),
            vmem((tp, slots, LANES), WIDE), vmem((tp, slots, LANES), WIDE),
            vmem((dp, slots // dp, LANES), WIDE), vmem((dp, slots // dp, LANES), WIDE),
            vmem((tp, dp, slots // dp, LANES), WIDE),
            pltpu.SemaphoreType.DMA((4,)),
            pltpu.SemaphoreType.DMA((12, tp)), pltpu.SemaphoreType.DMA((12, tp)),
            pltpu.SemaphoreType.DMA((6,)), pltpu.SemaphoreType.DMA((6,)),
        ],
        compiler_params=pltpu.CompilerParams(
            collective_id=0, has_side_effects=True, vmem_limit_bytes=60 * 2**20
        ),
    )(
        tokens.reshape(n, width), cotangent.reshape(n, width), dispatch_weight, w_in, w_out
    )
    grad_tokens, grad_router, grad_w_in, grad_w_out = outs
    return (grad_tokens.reshape(tokens.shape), grad_router.T, grad_w_in, grad_w_out)


def solution(mesh):
    return jax.shard_map(
        on_device,
        mesh=mesh,
        in_specs=(
            P("dp", "tensor", None),
            P("dp", "tensor", None),
            P(),
            P("dp", None, "tensor"),
            P("dp", "tensor", None),
        ),
        out_specs=(P("dp", "tensor", None), P(), P("dp", None, "tensor"), P("dp", "tensor", None)),
        check_vma=False,
    )
```

```python
import functools
import math

import jax
import jax.numpy as jnp
from jax import lax
from jax.experimental import pallas as pl
from jax.experimental.pallas import tpu as pltpu
from jax.sharding import PartitionSpec as P

WIDE = jnp.float32
LOW = jnp.bfloat16
MESH = pl.DeviceIdType.MESH
LANES = 128
LEAST = -3.0e38
PLANE = 4


def dot(a, b, over):
    return lax.dot_general(a, b, (over, ((), ())), preferred_element_type=WIDE)


def plain(a, b):
    return dot(a, b, ((1,), (0,)))


def rows_by_rows(a, b):
    return dot(a, b, ((1,), (1,)))


def columns_by_columns(a, b):
    return dot(a, b, ((0,), (0,)))


def iotas(shape):
    return lax.broadcasted_iota(jnp.int32, shape, 0), lax.broadcasted_iota(jnp.int32, shape, 1)


def kernel(
    tp, dp, images, own,
    tok_hbm, cot_hbm, router, w_in_hbm, w_out_hbm,
    grad_tok, grad_router, grad_in, grad_out,
    tok, cot, w_in, w_out, spread, weight, combine, dispatch, slot_slice,
    send_rows, recv_rows, send_slots, recv_slots, full, flat, sorted_rows, stats, stats_in,
    dots, dots_in, part, part_in, piece, piece_in, whole, final,
    local_sem, t_send, t_recv, d_send, d_recv, z_send, z_recv,
):
    me_t, me_d = lax.axis_index("tensor"), lax.axis_index("dp")
    n = tok.shape[0]
    group = own * images
    c = dp * group
    seq = n // images
    slots = dp * own
    half = c // own
    members, depth = PLANE * tp, dp // PLANE
    me_z, me_q = me_d // PLANE, lax.rem(me_d, PLANE)
    me_p = me_q * tp + me_t

    def copy_tensor(phase, k, src, dst, slot):
        to = lax.rem(me_t + k, tp)
        return pltpu.make_async_remote_copy(
            src_ref=src(to), dst_ref=dst(slot),
            send_sem=t_send.at[phase, k], recv_sem=t_recv.at[phase, k],
            device_id={"tensor": to}, device_id_type=MESH,
        )

    def start_tensor(phase, src, dst):
        for k in range(1, tp):
            copy_tensor(phase, k, src, dst, me_t).start()

    def await_tensor(phase, src, dst):
        for k in range(1, tp):
            copy_tensor(phase, k, src, dst, lax.rem(me_t + tp - k, tp)).wait_recv()

    def drain_tensor(phase, src, dst):
        for k in range(1, tp):
            copy_tensor(phase, k, src, dst, me_t).wait_send()

    def start_dp(phase, src, dst):
        def one(k, carry):
            to = lax.rem(me_d + k, dp)
            pltpu.make_async_remote_copy(
                src_ref=src(to), dst_ref=dst(me_d),
                send_sem=d_send.at[phase], recv_sem=d_recv.at[phase],
                device_id={"dp": to}, device_id_type=MESH,
            ).start()
            return carry
        lax.fori_loop(1, dp, one, 0)

    def all_dp(phase, out, into):
        return pltpu.make_async_remote_copy(
            src_ref=out.at[pl.ds(0, dp - 1)], dst_ref=into.at[pl.ds(0, dp - 1)],
            send_sem=d_send.at[phase], recv_sem=d_recv.at[phase],
            device_id={"dp": lax.rem(me_d + 1, dp)}, device_id_type=MESH,
        )

    STATS, DOTS = 8, 9
    rows_of = [
        (lot, lambda to, lot=lot: send_rows.at[lot, to], lambda s, lot=lot: recv_rows.at[lot, s])
        for lot in range(4)
    ]
    slots_of = [
        (4 + lot, lambda to, lot=lot: recv_slots.at[lot], lambda s, lot=lot: full.at[lot, s])
        for lot in range(4)
    ]
    stats_of = (STATS, lambda to: stats, lambda s: stats_in.at[s])
    dots_of = (DOTS, lambda to: dots, lambda s: dots_in.at[s])

    loads = [
        pltpu.make_async_copy(src, dst, local_sem.at[k])
        for k, (src, dst) in enumerate(
            [(tok_hbm, tok), (cot_hbm, cot), (w_in_hbm, w_in), (w_out_hbm, w_out)]
        )
    ]
    for load in loads:
        load.start()

    barrier = pltpu.get_barrier_semaphore()

    def greet(axis, me, size):
        def one(k, carry):
            pl.semaphore_signal(
                barrier, inc=1, device_id={axis: lax.rem(me + k, size)}, device_id_type=MESH
            )
            return carry
        lax.fori_loop(1, size, one, 0)

    greet("tensor", me_t, tp)
    greet("dp", me_d, dp)

    def to_member(k):
        member = lax.rem(me_p + k, members)
        q, t = member // tp, lax.rem(member, tp)
        return member, {"dp": me_z * PLANE + q, "tensor": t}

    def greet_plane(k, carry):
        q, t = lax.rem(me_q + 1 + k // (tp - 1), PLANE), lax.rem(me_t + 1 + lax.rem(k, tp - 1), tp)
        pl.semaphore_signal(
            barrier, inc=1, device_id={"dp": me_z * PLANE + q, "tensor": t}, device_id_type=MESH
        )
        return carry

    others = (PLANE - 1) * (tp - 1)
    lax.fori_loop(0, others, greet_plane, 0)

    row, col = iotas((c, slots))
    choose = jnp.where((row >= col * images) & (row < col * images + images), 1.0, 0.0).astype(LOW)
    spread[...] = plain(choose, router[...]).astype(LOW)
    loads[0].wait()
    row, col = iotas((c, n))
    begin = lax.rem(row, images) * seq
    ours = (col >= begin) & (col < begin + seq)
    masked = jnp.where(ours, rows_by_rows(spread[...], tok[...]), LEAST)
    top = jnp.max(masked, axis=1, keepdims=True)
    exponent = jnp.where(ours, jnp.exp(masked - top), 0.0)
    exponent_low = exponent.astype(LOW)
    weight[...] = exponent
    lane = iotas((c, LANES))[1]
    packed = jnp.where(
        lane == 0, top,
        jnp.where(
            lane == 1, jnp.sum(exponent, axis=1, keepdims=True),
            jnp.sum(exponent_low.astype(WIDE), axis=1, keepdims=True),
        ),
    )
    stats[...] = jnp.transpose(packed)[0:8, :]

    def cut(rows, lot):
        for t in range(tp):
            block = rows[:, t * LANES:(t + 1) * LANES].reshape(dp, group, LANES)
            send_rows[lot, t] = block.astype(LOW)

    cut(plain(exponent_low, tok[...]), 0)
    pl.semaphore_wait(barrier, tp + dp - 2 + others)
    start_tensor(*stats_of)
    start_tensor(*rows_of[0])

    loads[1].wait()
    best = jnp.max(masked, axis=0, keepdims=True)
    raised = jnp.where(ours, jnp.exp(masked - best), 0.0)
    share = raised / jnp.sum(raised, axis=0, keepdims=True)
    combine[...] = share
    cut(plain(share.astype(LOW), cot[...]), 1)
    start_tensor(*rows_of[1])

    await_tensor(*stats_of)
    stats_in[me_t] = stats[...]
    most = stats_in[0, 0:1]
    for s in range(1, tp):
        most = jnp.maximum(most, stats_in[s, 0:1])
    shrinks = [jnp.exp(stats_in[s, 0:1] - most) for s in range(tp)]
    total = sum(stats_in[s, 1:2] * shrinks[s] for s in range(tp))
    total_low = sum(stats_in[s, 2:3] * shrinks[s] for s in range(tp))
    lines = [shrink / total_low for shrink in shrinks]
    lines.append(jnp.exp(stats[0:1] - most) / total)
    line_row = iotas((LANES, c))[0]
    table = jnp.zeros((LANES, c), WIDE)
    for s, line in enumerate(lines):
        table = jnp.where(line_row == s, line, table)
    table = jnp.transpose(table)
    dispatch[...] = weight[...] * table[:, tp:tp + 1]

    def summed(lot, scales=None):
        await_tensor(*rows_of[lot])
        recv_rows[lot, me_t] = send_rows[lot, me_t]
        total_rows = None
        for s in range(tp):
            term = recv_rows[lot, s].astype(WIDE).reshape(c, LANES)
            if scales is not None:
                term = term * scales[:, s:s + 1]
            total_rows = term if total_rows is None else total_rows + term
        return total_rows

    def pass_on(total_rows, lot):
        send_slots[lot] = total_rows.reshape(dp, group, LANES).astype(LOW)
        start_dp(lot, lambda to: send_slots.at[lot, to], lambda s: recv_slots.at[lot, s])

    def gather(lot):
        all_dp(lot, send_slots.at[lot], recv_slots.at[lot]).wait_recv()
        recv_slots[lot, me_d] = send_slots[lot, me_d]
        start_tensor(*slots_of[lot])

    def assembled(lot):
        await_tensor(*slots_of[lot])
        full[lot, me_t] = recv_slots[lot]
        for t in range(tp):
            block = full[lot, t].astype(WIDE).reshape(c, LANES)
            flat[lot, :, t * LANES:(t + 1) * LANES] = block.astype(LOW)
        return flat[lot]

    slot_slice[...] = summed(0, table)
    pass_on(slot_slice[...], 0)
    pass_on(summed(1), 1)
    gather(0)
    gather(1)

    def matching(q, other):
        late = (q >= half).astype(jnp.int32)
        image = lax.rem(q, images)
        return other == own * (q - late * half - image) + image + late * images

    row, col = iotas((c, c))
    sort = jnp.where(matching(row, col), 1.0, 0.0).astype(LOW)
    unsort = jnp.where(matching(col, row), 1.0, 0.0).astype(LOW)
    for load in loads[2:]:
        load.wait()
    root = math.sqrt(2.0 / math.pi)
    sorted_rows[0] = plain(sort, assembled(0)).astype(LOW)
    hidden, slope, results = [], [], []
    for e in range(own):
        pre = plain(sorted_rows[0, e * half:(e + 1) * half], w_in[e])
        square = pre * pre
        bent = jnp.tanh(root * (pre + 0.044715 * (square * pre)))
        hidden.append((0.5 * pre * (1.0 + bent)).astype(LOW))
        slope.append(
            0.5 * (1.0 + bent)
            + 0.5 * pre * (1.0 - bent * bent) * (root * (1.0 + 3.0 * 0.044715 * square))
        )
        results.append(plain(hidden[e], w_out[e]).astype(LOW))
    cut(plain(unsort, jnp.concatenate(results)), 2)
    start_tensor(*rows_of[2])
    sorted_rows[1] = plain(sort, assembled(1)).astype(LOW)
    grad_pre, results = [], []
    for e in range(own):
        grad_hidden = rows_by_rows(sorted_rows[1, e * half:(e + 1) * half], w_out[e])
        grad_pre.append((slope[e] * grad_hidden).astype(LOW))
        results.append(rows_by_rows(grad_pre[e], w_in[e]).astype(LOW))
    cut(plain(unsort, jnp.concatenate(results)), 3)
    start_tensor(*rows_of[3])
    for e in range(own):
        here = slice(e * half, (e + 1) * half)
        grad_out[e] = columns_by_columns(hidden[e], sorted_rows[1, here]).astype(LOW)
        grad_in[e] = columns_by_columns(sorted_rows[0, here], grad_pre[e]).astype(LOW)
    pass_on(summed(2), 2)
    pass_on(summed(3), 3)
    gather(2)
    gather(3)
    products = recv_slots[3].astype(WIDE).reshape(c, LANES) * slot_slice[...]
    own_dots = jnp.broadcast_to(jnp.sum(products, axis=1, keepdims=True), (c, LANES))
    dots[...] = jnp.transpose(own_dots)[0:8, :]
    start_tensor(*dots_of)

    slot_out = assembled(2)
    share = combine[...]
    grad_share = rows_by_rows(slot_out, cot[...])
    row_dot = jnp.sum(grad_share * share, axis=0, keepdims=True)
    from_share = share * (grad_share - row_dot)
    slot_grad = assembled(3)
    grad_weight = rows_by_rows(slot_grad, tok[...])
    await_tensor(*dots_of)
    dots_in[me_t] = dots[...]
    dot_line = dots_in[0, 0:1]
    for s in range(1, tp):
        dot_line = dot_line + dots_in[s, 0:1]
    column_dot = jnp.transpose(jnp.broadcast_to(dot_line, (LANES, c)))[:, 0:1]
    spots = dispatch[...]
    grad_logits = (from_share + spots * (grad_weight - column_dot)).astype(LOW)
    row, col = iotas((slots, c))
    fold = jnp.where((col >= row * images) & (col < row * images + images), 1.0, 0.0).astype(LOW)
    by_slot = plain(fold, grad_logits).astype(LOW)
    local_router = plain(by_slot, tok[...])
    high = slots // PLANE
    for q in range(PLANE):
        for t in range(tp):
            part[q * tp + t] = local_router[
                q * high:(q + 1) * high, t * LANES:(t + 1) * LANES
            ].astype(LOW)

    def send_part(k, carry):
        member, where = to_member(k)
        pltpu.make_async_remote_copy(
            src_ref=part.at[member], dst_ref=part_in.at[me_p],
            send_sem=d_send.at[4], recv_sem=d_recv.at[4],
            device_id=where, device_id_type=MESH,
        ).start()
        return carry

    lax.fori_loop(1, members, send_part, 0)
    grad_tok[...] = (
        columns_by_columns(spots.astype(LOW), slot_grad)
        + columns_by_columns(grad_logits, spread[...])
    ).astype(LOW)

    def all_members(phase, out, into):
        return pltpu.make_async_remote_copy(
            src_ref=out.at[pl.ds(0, members - 1)], dst_ref=into.at[pl.ds(0, members - 1)],
            send_sem=d_send.at[phase], recv_sem=d_recv.at[phase],
            device_id=to_member(1)[1], device_id_type=MESH,
        )

    all_members(4, part, part_in).wait_recv()
    part_in[me_p] = part[me_p]
    piece[...] = jnp.sum(part_in[...].astype(WIDE), axis=0)

    def piece_copy(k, slot):
        return pltpu.make_async_remote_copy(
            src_ref=piece, dst_ref=piece_in.at[slot],
            send_sem=z_send.at[k], recv_sem=z_recv.at[k],
            device_id={"dp": lax.rem(me_z + k, depth) * PLANE + me_q}, device_id_type=MESH,
        )

    for k in range(1, depth):
        piece_copy(k, me_z).start()
    for k in range(1, depth):
        piece_copy(k, lax.rem(me_z + depth - k, depth)).wait_recv()
    piece_in[me_z] = piece[...]
    final[...] = jnp.sum(piece_in[...], axis=0).astype(LOW)

    def send_final(k, carry):
        pltpu.make_async_remote_copy(
            src_ref=final, dst_ref=whole.at[me_p],
            send_sem=d_send.at[5], recv_sem=d_recv.at[5],
            device_id=to_member(k)[1], device_id_type=MESH,
        ).start()
        return carry

    lax.fori_loop(1, members, send_final, 0)
    all_members(5, whole, whole).wait_recv()
    whole[me_p] = final[...]
    for q in range(PLANE):
        for t in range(tp):
            grad_router[q * high:(q + 1) * high, t * LANES:(t + 1) * LANES] = (
                whole[q * tp + t].astype(WIDE)
            )

    for phase in [*rows_of, *slots_of, stats_of, dots_of]:
        drain_tensor(*phase)
    for lot in range(4):
        all_dp(lot, send_slots.at[lot], recv_slots.at[lot]).wait_send()
    for k in range(1, depth):
        piece_copy(k, me_z).wait_send()
    all_members(4, part, part_in).wait_send()
    all_members(5, whole, whole).wait_send()


def finish(*refs):
    count = (len(refs) - 1) // 2
    copies = [
        pltpu.make_async_copy(refs[k], refs[count + k], refs[-1].at[k]) for k in range(count)
    ]
    for copy in copies:
        copy.start()
    for copy in copies:
        copy.wait()


def on_device(tokens, cotangent, dispatch_weight, w_in, w_out):
    tp, dp = lax.axis_size("tensor"), lax.axis_size("dp")
    images, seq, width = tokens.shape
    own, _, inner = w_in.shape
    n, slots, group = images * seq, dp * own, own * images
    c = dp * group
    members, high = PLANE * tp, slots // PLANE
    vmem, hbm = pltpu.VMEM, pl.BlockSpec(memory_space=pltpu.HBM)
    here = pl.BlockSpec(memory_space=pltpu.VMEM)
    shapes = [((n, width), LOW), ((slots, width), WIDE), (w_in.shape, LOW), (w_out.shape, LOW)]
    outs = pl.pallas_call(
        functools.partial(kernel, tp, dp, images, own),
        name="moe_back",
        out_shape=tuple(vmem(*shape) for shape in shapes),
        in_specs=[hbm, hbm, here, hbm, hbm],
        out_specs=(here,) * 4,
        scratch_shapes=[
            vmem((n, width), LOW), vmem((n, width), LOW),
            vmem(w_in.shape, LOW), vmem(w_out.shape, LOW),
            vmem((c, width), LOW),
            vmem((c, n), WIDE), vmem((c, n), WIDE), vmem((c, n), WIDE),
            vmem((c, LANES), WIDE),
            vmem((4, tp, dp, group, LANES), LOW), vmem((4, tp, dp, group, LANES), LOW),
            vmem((4, dp, group, LANES), LOW), vmem((4, dp, group, LANES), LOW),
            vmem((4, tp, dp, group, LANES), LOW),
            vmem((4, c, width), LOW), vmem((2, c, width), LOW),
            vmem((8, c), WIDE), vmem((tp, 8, c), WIDE),
            vmem((8, c), WIDE), vmem((tp, 8, c), WIDE),
            vmem((members, high, LANES), LOW), vmem((members, high, LANES), LOW),
            vmem((high, LANES), WIDE), vmem((dp // PLANE, high, LANES), WIDE),
            vmem((members, high, LANES), LOW), vmem((high, LANES), LOW),
            pltpu.SemaphoreType.DMA((4,)),
            pltpu.SemaphoreType.DMA((10, tp)), pltpu.SemaphoreType.DMA((10, tp)),
            pltpu.SemaphoreType.DMA((6,)), pltpu.SemaphoreType.DMA((6,)),
            pltpu.SemaphoreType.DMA((dp // PLANE,)), pltpu.SemaphoreType.DMA((dp // PLANE,)),
        ],
        compiler_params=pltpu.CompilerParams(
            collective_id=0, has_side_effects=True, vmem_limit_bytes=61400000
        ),
    )(
        tokens.reshape(n, width), cotangent.reshape(n, width), dispatch_weight.T, w_in, w_out
    )
    grad_tokens, grad_router, grad_w_in, grad_w_out = pl.pallas_call(
        finish,
        name="finish",
        out_shape=tuple(jax.ShapeDtypeStruct(*shape) for shape in shapes),
        in_specs=[here] * 4,
        out_specs=(hbm,) * 4,
        scratch_shapes=[pltpu.SemaphoreType.DMA((4,))],
        compiler_params=pltpu.CompilerParams(vmem_limit_bytes=4 * 2**20),
    )(*outs)
    return (grad_tokens.reshape(tokens.shape), grad_router.T, grad_w_in, grad_w_out)


def solution(mesh):
    return jax.shard_map(
        on_device,
        mesh=mesh,
        in_specs=(
            P("dp", "tensor", None),
            P("dp", "tensor", None),
            P(),
            P("dp", None, "tensor"),
            P("dp", "tensor", None),
        ),
        out_specs=(P("dp", "tensor", None), P(), P("dp", None, "tensor"), P("dp", "tensor", None)),
        check_vma=False,
    )
```

```python
import functools
import math

import jax
import jax.numpy as jnp
from jax import lax
from jax.experimental import pallas as pl
from jax.experimental.pallas import tpu as pltpu
from jax.sharding import PartitionSpec as P

WIDE = jnp.float32
LOW = jnp.bfloat16
MESH = pl.DeviceIdType.MESH
LANES = 128
LEAST = -3.0e38
PLANE = 4


def dot(a, b, over):
    return lax.dot_general(a, b, (over, ((), ())), preferred_element_type=WIDE)


def plain(a, b):
    return dot(a, b, ((1,), (0,)))


def rows_by_rows(a, b):
    return dot(a, b, ((1,), (1,)))


def columns_by_columns(a, b):
    return dot(a, b, ((0,), (0,)))


def iotas(shape):
    return lax.broadcasted_iota(jnp.int32, shape, 0), lax.broadcasted_iota(jnp.int32, shape, 1)


def kernel(
    tp, dp, images, own,
    router_hbm, tok_hbm, cot_hbm, w_in_hbm, w_out_hbm,
    grad_tok, grad_router, grad_in, grad_out,
    router, tok, cot, w_in, w_out, spread, weight, combine, dispatch, slot_slice,
    send_rows, recv_rows, send_slots, recv_slots, full, flat, hidden, grad_pre, stats, stats_in,
    dots, dots_in, part, part_in, piece, piece_in, whole, final,
    local_sem, t_send, t_recv, d_send, d_recv, z_send, z_recv,
):
    me_t, me_d = lax.axis_index("tensor"), lax.axis_index("dp")
    n = tok.shape[0]
    group = own * images
    c = dp * group
    seq = n // images
    slots = dp * own
    half = c // own
    members, depth = PLANE * tp, dp // PLANE
    me_z, me_q = me_d // PLANE, lax.rem(me_d, PLANE)
    me_p = me_q * tp + me_t

    def copy_tensor(phase, k, src, dst, slot):
        to = lax.rem(me_t + k, tp)
        return pltpu.make_async_remote_copy(
            src_ref=src(to), dst_ref=dst(slot),
            send_sem=t_send.at[phase, k], recv_sem=t_recv.at[phase, k],
            device_id={"tensor": to}, device_id_type=MESH,
        )

    def start_tensor(phase, src, dst):
        for k in range(1, tp):
            copy_tensor(phase, k, src, dst, me_t).start()

    def await_tensor(phase, src, dst):
        for k in range(1, tp):
            copy_tensor(phase, k, src, dst, lax.rem(me_t + tp - k, tp)).wait_recv()

    def drain_tensor(phase, src, dst):
        for k in range(1, tp):
            copy_tensor(phase, k, src, dst, me_t).wait_send()

    def outward(k, size):
        return size // 2 + (2 * lax.rem(k, 2) - 1) * ((k + 1) // 2)

    def start_dp(phase, src, dst):
        def one(k, carry):
            to = lax.rem(me_d + outward(k, dp), dp)
            pltpu.make_async_remote_copy(
                src_ref=src(to), dst_ref=dst(me_d),
                send_sem=d_send.at[phase], recv_sem=d_recv.at[phase],
                device_id={"dp": to}, device_id_type=MESH,
            ).start()
            return carry
        lax.fori_loop(0, dp - 1, one, 0)

    def all_dp(phase, out, into):
        return pltpu.make_async_remote_copy(
            src_ref=out.at[pl.ds(0, dp - 1)], dst_ref=into.at[pl.ds(0, dp - 1)],
            send_sem=d_send.at[phase], recv_sem=d_recv.at[phase],
            device_id={"dp": lax.rem(me_d + 1, dp)}, device_id_type=MESH,
        )

    lots = [(turn, kind, e) for turn in range(2) for kind in range(2) for e in range(own)]
    number = {lot: k for k, lot in enumerate(lots)}
    STATS, DOTS = 2 * len(lots), 2 * len(lots) + 1
    rows_of = [
        (k, lambda to, k=k: send_rows.at[k, to], lambda s, k=k: recv_rows.at[k, s])
        for k in range(len(lots))
    ]
    slots_of = [
        (len(lots) + k, lambda to, k=k: recv_slots.at[k], lambda s, k=k: full.at[k, s])
        for k in range(len(lots))
    ]
    stats_of = (STATS, lambda to: stats, lambda s: stats_in.at[s])
    dots_of = (DOTS, lambda to: dots, lambda s: dots_in.at[s])

    loads = [
        pltpu.make_async_copy(src, dst, local_sem.at[k])
        for k, (src, dst) in enumerate(
            [
                (router_hbm, router), (tok_hbm, tok), (cot_hbm, cot),
                (w_in_hbm, w_in), (w_out_hbm, w_out),
            ]
        )
    ]
    for load in loads:
        load.start()

    barrier = pltpu.get_barrier_semaphore()

    def greet_dp(k, carry):
        pl.semaphore_signal(
            barrier, inc=1, device_id={"dp": lax.rem(me_d + outward(k, dp), dp)},
            device_id_type=MESH,
        )
        return carry

    lax.fori_loop(0, dp - 1, greet_dp, 0)

    def to_member(k):
        member = lax.rem(me_p + k, members)
        q, t = member // tp, lax.rem(member, tp)
        return member, {"dp": me_z * PLANE + q, "tensor": t}

    def greet_plane(k, carry):
        q, t = lax.rem(me_q + 1 + k // (tp - 1), PLANE), lax.rem(me_t + 1 + lax.rem(k, tp - 1), tp)
        pl.semaphore_signal(
            barrier, inc=1, device_id={"dp": me_z * PLANE + q, "tensor": t}, device_id_type=MESH
        )
        return carry

    others = (PLANE - 1) * (tp - 1)
    lax.fori_loop(0, others, greet_plane, 0)
    for k in range(1, tp):
        pl.semaphore_signal(
            barrier, inc=1, device_id={"tensor": lax.rem(me_t + k, tp)}, device_id_type=MESH
        )

    def belongs(slot, at):
        e = lax.rem(slot, own)
        first = e * half + (slot - e) * (images // own)
        return (at >= first) & (at < first + images)

    row, col = iotas((c, slots))
    choose = jnp.where(belongs(col, row), 1.0, 0.0).astype(LOW)
    loads[0].wait()
    spread[...] = plain(choose, router[...]).astype(LOW)
    loads[1].wait()
    row, col = iotas((c, n))
    begin = lax.rem(row, images) * seq
    ours = (col >= begin) & (col < begin + seq)
    masked = jnp.where(ours, rows_by_rows(spread[...], tok[...]), LEAST)
    top = jnp.max(masked, axis=1, keepdims=True)
    exponent = jnp.where(ours, jnp.exp(masked - top), 0.0)
    exponent_low = exponent.astype(LOW)
    weight[...] = exponent
    lane = iotas((c, LANES))[1]
    packed = jnp.where(
        lane == 0, top,
        jnp.where(
            lane == 1, jnp.sum(exponent, axis=1, keepdims=True),
            jnp.sum(exponent_low.astype(WIDE), axis=1, keepdims=True),
        ),
    )
    stats[...] = jnp.transpose(packed)[0:8, :]

    def cut(rows, lot):
        for t in range(tp):
            block = rows[:, t * LANES:(t + 1) * LANES].reshape(dp, images, LANES)
            send_rows[number[lot], t] = block.astype(LOW)

    def begin_sum(rows, lot):
        cut(rows, lot)
        start_tensor(*rows_of[number[lot]])

    cut(plain(exponent_low[0:half], tok[...]), (0, 0, 0))
    pl.semaphore_wait(barrier, tp + dp - 2 + others)
    start_tensor(*stats_of)
    start_tensor(*rows_of[0])
    for e in range(1, own):
        begin_sum(plain(exponent_low[e * half:(e + 1) * half], tok[...]), (0, 0, e))

    loads[2].wait()
    best = jnp.max(masked, axis=0, keepdims=True)
    raised = jnp.where(ours, jnp.exp(masked - best), 0.0)
    share = raised / jnp.sum(raised, axis=0, keepdims=True)
    combine[...] = share
    share_low = share.astype(LOW)
    for e in range(own):
        begin_sum(plain(share_low[e * half:(e + 1) * half], cot[...]), (0, 1, e))

    await_tensor(*stats_of)
    stats_in[me_t] = stats[...]
    most = stats_in[0, 0:1]
    for s in range(1, tp):
        most = jnp.maximum(most, stats_in[s, 0:1])
    shrinks = [jnp.exp(stats_in[s, 0:1] - most) for s in range(tp)]
    total = sum(stats_in[s, 1:2] * shrinks[s] for s in range(tp))
    total_low = sum(stats_in[s, 2:3] * shrinks[s] for s in range(tp))
    lines = [shrink / total_low for shrink in shrinks]
    lines.append(jnp.exp(stats[0:1] - most) / total)
    line_row = iotas((LANES, c))[0]
    table = jnp.zeros((LANES, c), WIDE)
    for s, line in enumerate(lines):
        table = jnp.where(line_row == s, line, table)
    table = jnp.transpose(table)
    dispatch[...] = weight[...] * table[:, tp:tp + 1]

    def pass_on(lot):
        k, e = number[lot], lot[2]
        await_tensor(*rows_of[k])
        recv_rows[k, me_t] = send_rows[k, me_t]
        total_rows = None
        for s in range(tp):
            term = recv_rows[k, s].astype(WIDE).reshape(half, LANES)
            if lot[:2] == (0, 0):
                term = term * table[e * half:(e + 1) * half, s:s + 1]
            total_rows = term if total_rows is None else total_rows + term
        if lot[:2] == (0, 0):
            slot_slice[e * half:(e + 1) * half] = total_rows
        send_slots[k] = total_rows.reshape(dp, images, LANES).astype(LOW)
        start_dp(k, lambda to: send_slots.at[k, to], lambda s: recv_slots.at[k, s])

    def gather(lot):
        k = number[lot]
        all_dp(k, send_slots.at[k], recv_slots.at[k]).wait_recv()
        recv_slots[k, me_d] = send_slots[k, me_d]
        start_tensor(*slots_of[k])

    def assembled(lot):
        k, (turn, kind, e) = number[lot], lot
        await_tensor(*slots_of[k])
        full[k, me_t] = recv_slots[k]
        for t in range(tp):
            block = full[k, t].astype(WIDE).reshape(half, LANES)
            flat[turn, kind, e * half:(e + 1) * half, t * LANES:(t + 1) * LANES] = (
                block.astype(LOW)
            )
        return flat[turn, kind, e * half:(e + 1) * half]

    root = math.sqrt(2.0 / math.pi)
    slope = {}

    def expert_out(e):
        pre = plain(assembled((0, 0, e)), w_in[e])
        square = pre * pre
        bent = jnp.tanh(root * (pre + 0.044715 * (square * pre)))
        hidden[e] = (0.5 * pre * (1.0 + bent)).astype(LOW)
        slope[e] = 0.5 * (1.0 + bent) + 0.5 * pre * (1.0 - bent * bent) * (
            root * (1.0 + 3.0 * 0.044715 * square)
        )
        begin_sum(plain(hidden[e], w_out[e]), (1, 0, e))

    def expert_back(e):
        grad_hidden = rows_by_rows(assembled((0, 1, e)), w_out[e])
        grad_pre[e] = (slope[e] * grad_hidden).astype(LOW)
        begin_sum(rows_by_rows(grad_pre[e], w_in[e]), (1, 1, e))

    pass_on((0, 0, 0))
    pass_on((0, 0, 1))
    pass_on((0, 1, 0))
    gather((0, 0, 0))
    pass_on((0, 1, 1))
    gather((0, 0, 1))
    gather((0, 1, 0))
    for load in loads[3:]:
        load.wait()
    gather((0, 1, 1))
    expert_out(0)
    expert_out(1)
    expert_back(0)
    expert_back(1)
    pass_on((1, 0, 0))
    pass_on((1, 0, 1))
    pass_on((1, 1, 0))
    gather((1, 0, 0))
    pass_on((1, 1, 1))
    gather((1, 0, 1))
    gather((1, 1, 0))
    gather((1, 1, 1))
    products = jnp.concatenate([
        recv_slots[number[(1, 1, e)]].astype(WIDE).reshape(half, LANES) for e in range(own)
    ]) * slot_slice[...]
    own_dots = jnp.broadcast_to(jnp.sum(products, axis=1, keepdims=True), (c, LANES))
    dots[...] = jnp.transpose(own_dots)[0:8, :]
    start_tensor(*dots_of)
    for e in range(own):
        here = slice(e * half, (e + 1) * half)
        grad_out[e] = columns_by_columns(hidden[e], flat[0, 1, here]).astype(LOW)
        grad_in[e] = columns_by_columns(flat[0, 0, here], grad_pre[e]).astype(LOW)

    share = combine[...]
    grad_share = jnp.concatenate(
        [rows_by_rows(assembled((1, 0, e)), cot[...]) for e in range(own)]
    )
    row_dot = jnp.sum(grad_share * share, axis=0, keepdims=True)
    from_share = share * (grad_share - row_dot)
    grad_weight = jnp.concatenate(
        [rows_by_rows(assembled((1, 1, e)), tok[...]) for e in range(own)]
    )
    slot_grad = flat[1, 1]
    await_tensor(*dots_of)
    dots_in[me_t] = dots[...]
    dot_line = dots_in[0, 0:1]
    for s in range(1, tp):
        dot_line = dot_line + dots_in[s, 0:1]
    column_dot = jnp.transpose(jnp.broadcast_to(dot_line, (LANES, c)))[:, 0:1]
    spots = dispatch[...]
    grad_logits = (from_share + spots * (grad_weight - column_dot)).astype(LOW)
    row, col = iotas((slots, c))
    fold = jnp.where(belongs(row, col), 1.0, 0.0).astype(LOW)
    by_slot = plain(fold, grad_logits).astype(LOW)
    local_router = plain(by_slot, tok[...])
    high = slots // PLANE
    for q in range(PLANE):
        for t in range(tp):
            part[q * tp + t] = local_router[
                q * high:(q + 1) * high, t * LANES:(t + 1) * LANES
            ].astype(LOW)

    def send_part(k, carry):
        member, where = to_member(k)
        pltpu.make_async_remote_copy(
            src_ref=part.at[member], dst_ref=part_in.at[me_p],
            send_sem=d_send.at[8], recv_sem=d_recv.at[8],
            device_id=where, device_id_type=MESH,
        ).start()
        return carry

    lax.fori_loop(1, members, send_part, 0)
    grad_tok[...] = (
        columns_by_columns(spots.astype(LOW), slot_grad)
        + columns_by_columns(grad_logits, spread[...])
    ).astype(LOW)

    def all_members(phase, out, into):
        return pltpu.make_async_remote_copy(
            src_ref=out.at[pl.ds(0, members - 1)], dst_ref=into.at[pl.ds(0, members - 1)],
            send_sem=d_send.at[phase], recv_sem=d_recv.at[phase],
            device_id=to_member(1)[1], device_id_type=MESH,
        )

    all_members(8, part, part_in).wait_recv()
    part_in[me_p] = part[me_p]
    piece[...] = jnp.sum(part_in[...].astype(WIDE), axis=0)

    def piece_copy(k, slot):
        return pltpu.make_async_remote_copy(
            src_ref=piece, dst_ref=piece_in.at[slot],
            send_sem=z_send.at[k], recv_sem=z_recv.at[k],
            device_id={"dp": lax.rem(me_z + k, depth) * PLANE + me_q}, device_id_type=MESH,
        )

    for k in range(1, depth):
        piece_copy(k, me_z).start()
    for k in range(1, depth):
        piece_copy(k, lax.rem(me_z + depth - k, depth)).wait_recv()
    piece_in[me_z] = piece[...]
    final[...] = jnp.sum(piece_in[...], axis=0).astype(LOW)

    def send_final(k, carry):
        pltpu.make_async_remote_copy(
            src_ref=final, dst_ref=whole.at[me_p],
            send_sem=d_send.at[9], recv_sem=d_recv.at[9],
            device_id=to_member(k)[1], device_id_type=MESH,
        ).start()
        return carry

    lax.fori_loop(1, members, send_final, 0)
    all_members(9, whole, whole).wait_recv()
    whole[me_p] = final[...]
    for q in range(PLANE):
        for t in range(tp):
            grad_router[q * high:(q + 1) * high, t * LANES:(t + 1) * LANES] = (
                whole[q * tp + t].astype(WIDE)
            )

    for phase in [*rows_of, *slots_of, stats_of, dots_of]:
        drain_tensor(*phase)
    for k in range(len(lots)):
        all_dp(k, send_slots.at[k], recv_slots.at[k]).wait_send()
    for k in range(1, depth):
        piece_copy(k, me_z).wait_send()
    all_members(8, part, part_in).wait_send()
    all_members(9, whole, whole).wait_send()


def finish(*refs):
    count = (len(refs) - 1) // 2
    copies = [
        pltpu.make_async_copy(refs[k], refs[count + k], refs[-1].at[k]) for k in range(count)
    ]
    for copy in copies:
        copy.start()
    for copy in copies:
        copy.wait()


def on_device(tokens, cotangent, dispatch_weight, w_in, w_out):
    tp, dp = lax.axis_size("tensor"), lax.axis_size("dp")
    images, seq, width = tokens.shape
    own, _, inner = w_in.shape
    n, slots, group = images * seq, dp * own, own * images
    c = dp * group
    members, high, lots = PLANE * tp, slots // PLANE, 4 * own
    vmem, hbm = pltpu.VMEM, pl.BlockSpec(memory_space=pltpu.HBM)
    here = pl.BlockSpec(memory_space=pltpu.VMEM)
    shapes = [((n, width), LOW), ((slots, width), WIDE), (w_in.shape, LOW), (w_out.shape, LOW)]
    outs = pl.pallas_call(
        functools.partial(kernel, tp, dp, images, own),
        name="moe_back",
        out_shape=tuple(vmem(*shape) for shape in shapes),
        in_specs=[hbm] * 5,
        out_specs=(here,) * 4,
        scratch_shapes=[
            vmem((slots, width), LOW), vmem((n, width), LOW), vmem((n, width), LOW),
            vmem(w_in.shape, LOW), vmem(w_out.shape, LOW),
            vmem((c, width), LOW),
            vmem((c, n), WIDE), vmem((c, n), WIDE), vmem((c, n), WIDE),
            vmem((c, LANES), WIDE),
            vmem((lots, tp, dp, images, LANES), LOW), vmem((lots, tp, dp, images, LANES), LOW),
            vmem((lots, dp, images, LANES), LOW), vmem((lots, dp, images, LANES), LOW),
            vmem((lots, tp, dp, images, LANES), LOW),
            vmem((2, 2, c, width), LOW),
            vmem((own, c // own, inner), LOW), vmem((own, c // own, inner), LOW),
            vmem((8, c), WIDE), vmem((tp, 8, c), WIDE),
            vmem((8, c), WIDE), vmem((tp, 8, c), WIDE),
            vmem((members, high, LANES), LOW), vmem((members, high, LANES), LOW),
            vmem((high, LANES), WIDE), vmem((dp // PLANE, high, LANES), WIDE),
            vmem((members, high, LANES), LOW), vmem((high, LANES), LOW),
            pltpu.SemaphoreType.DMA((5,)),
            pltpu.SemaphoreType.DMA((2 * lots + 2, tp)), pltpu.SemaphoreType.DMA((2 * lots + 2, tp)),
            pltpu.SemaphoreType.DMA((lots + 2,)), pltpu.SemaphoreType.DMA((lots + 2,)),
            pltpu.SemaphoreType.DMA((dp // PLANE,)), pltpu.SemaphoreType.DMA((dp // PLANE,)),
        ],
        compiler_params=pltpu.CompilerParams(
            collective_id=0, has_side_effects=True, vmem_limit_bytes=61400000
        ),
    )(
        dispatch_weight.T, tokens.reshape(n, width), cotangent.reshape(n, width), w_in, w_out
    )
    grad_tokens, grad_router, grad_w_in, grad_w_out = pl.pallas_call(
        finish,
        name="finish",
        out_shape=tuple(jax.ShapeDtypeStruct(*shape) for shape in shapes),
        in_specs=[here] * 4,
        out_specs=(hbm,) * 4,
        scratch_shapes=[pltpu.SemaphoreType.DMA((4,))],
        compiler_params=pltpu.CompilerParams(vmem_limit_bytes=4 * 2**20),
    )(*outs)
    return (grad_tokens.reshape(tokens.shape), grad_router.T, grad_w_in, grad_w_out)


def solution(mesh):
    return jax.shard_map(
        on_device,
        mesh=mesh,
        in_specs=(
            P("dp", "tensor", None),
            P("dp", "tensor", None),
            P(),
            P("dp", None, "tensor"),
            P("dp", "tensor", None),
        ),
        out_specs=(P("dp", "tensor", None), P(), P("dp", None, "tensor"), P("dp", "tensor", None)),
        check_vma=False,
    )
```

```python
import functools
import math

import jax
import jax.numpy as jnp
from jax import lax
from jax.experimental import pallas as pl
from jax.experimental.pallas import tpu as pltpu
from jax.sharding import PartitionSpec as P

WIDE = jnp.float32
LOW = jnp.bfloat16
MESH = pl.DeviceIdType.MESH
LANES = 128
LEAST = -3.0e38
PLANE = 4


def dot(a, b, over):
    return lax.dot_general(a, b, (over, ((), ())), preferred_element_type=WIDE)


def plain(a, b):
    return dot(a, b, ((1,), (0,)))


def rows_by_rows(a, b):
    return dot(a, b, ((1,), (1,)))


def columns_by_columns(a, b):
    return dot(a, b, ((0,), (0,)))


def iotas(shape):
    return lax.broadcasted_iota(jnp.int32, shape, 0), lax.broadcasted_iota(jnp.int32, shape, 1)


def kernel(
    tp, dp, images, own,
    router_hbm, tok_hbm, cot_hbm, w_in_hbm, w_out_hbm,
    grad_tok, grad_router, grad_in, grad_out,
    router, tok, cot, w_in, w_out, spread, weight, combine, dispatch, slot_slice,
    out_send, out_recv, back_send, back_recv, send_slots, slots_out, slots_back,
    full_out, full_back, flat, hidden, grad_pre,
    stats, stats_in,
    dots, dots_in, part, part_in, piece, piece_in, whole, final,
    local_sem, t_send, t_recv, p_send, p_recv, z_send, z_recv,
):
    me_t, me_d = lax.axis_index("tensor"), lax.axis_index("dp")
    n = tok.shape[0]
    group = own * images
    c = dp * group
    seq = n // images
    slots = dp * own
    half = c // own
    members, depth = PLANE * tp, dp // PLANE
    me_z, me_q = me_d // PLANE, lax.rem(me_d, PLANE)
    me_p = me_q * tp + me_t

    def copy_tensor(phase, k, src, dst, slot):
        to = lax.rem(me_t + k, tp)
        return pltpu.make_async_remote_copy(
            src_ref=src(to), dst_ref=dst(slot),
            send_sem=t_send.at[phase, k], recv_sem=t_recv.at[phase, k],
            device_id={"tensor": to}, device_id_type=MESH,
        )

    def start_tensor(phase, src, dst):
        for k in sorted(range(1, tp), key=lambda k: -min(k, tp - k)):
            copy_tensor(phase, k, src, dst, me_t).start()

    def before(k):
        return lax.rem(me_t + tp - k, tp)

    def await_one(k, phase, src, dst):
        copy_tensor(phase, k, src, dst, before(k)).wait_recv()

    def await_tensor(phase, src, dst):
        for k in range(1, tp):
            await_one(k, phase, src, dst)

    def drain_tensor(phase, src, dst):
        for k in range(1, tp):
            copy_tensor(phase, k, src, dst, me_t).wait_send()

    def remote(src, dst, send_sem, recv_sem, where):
        return pltpu.make_async_remote_copy(
            src_ref=src, dst_ref=dst, send_sem=send_sem, recv_sem=recv_sem,
            device_id=where, device_id_type=MESH,
        )

    near = [
        (lax.rem(me_q + jq, PLANE), lax.rem(me_t + jt, tp))
        for jt in sorted(range(tp), key=lambda jt: -min(jt, tp - jt))
        for jq in sorted(range(PLANE), key=lambda jq: -min(jq, PLANE - jq))
        if (jq, jt) != (0, 0)
    ]

    def start_plane(phase, src, dst):
        for q, t in near:
            remote(
                src(q, t), dst, p_send.at[phase], p_recv.at[phase],
                {"dp": me_z * PLANE + q, "tensor": t},
            ).start()

    def all_plane(phase, blocks):
        few = pl.ds(0, members - 1)
        q, t = near[0]
        return remote(
            blocks.at[few], blocks.at[few], p_send.at[phase], p_recv.at[phase],
            {"dp": me_z * PLANE + q, "tensor": t},
        )

    def z_copy(phase, k, src, dst, slot):
        to = lax.rem(me_z + k, depth)
        return remote(
            src(to), dst(slot), z_send.at[phase, k], z_recv.at[phase, k],
            {"dp": to * PLANE + me_q},
        )

    def start_z(phase, src, dst):
        for k in sorted(range(1, depth), key=lambda k: -min(k, depth - k)):
            z_copy(phase, k, src, dst, me_z).start()

    def await_z(phase, src, dst):
        for k in range(1, depth):
            z_copy(phase, k, src, dst, lax.rem(me_z + depth - k, depth)).wait_recv()

    def drain_z(phase, src, dst):
        for k in range(1, depth):
            z_copy(phase, k, src, dst, me_z).wait_send()

    lots = [(turn, kind, e) for turn in range(2) for kind in range(2) for e in range(own)]
    number = {lot: k for k, lot in enumerate(lots)}
    STATS, DOTS = len(lots), len(lots) + 1
    ways = len(lots) // 2
    tensor_of = [
        (k, lambda to, k=k: out_send.at[k, to], lambda s, k=k: out_recv.at[k, s])
        for k in range(ways)
    ] + [
        (ways + k, lambda to, k=k: slots_back.at[k], lambda s, k=k: full_back.at[k, s])
        for k in range(ways)
    ]
    plane_of = [
        (k, lambda q, t, k=k: slots_out.at[k, q], full_out.at[k, me_p]) for k in range(ways)
    ] + [
        (ways + k, lambda q, t, k=k: back_send.at[k, q * tp + t], back_recv.at[k, me_p])
        for k in range(ways)
    ]
    z_of = [
        (k, lambda to, k=k: send_slots.at[k, to], lambda s, k=k: slots_out.at[k, :, s])
        for k in range(ways)
    ] + [
        (k, lambda to, k=k: send_slots.at[k, to], lambda s, k=k: slots_back.at[k - ways, s])
        for k in range(ways, 2 * ways)
    ]
    PART, WHOLE, PIECE = 2 * ways, 2 * ways + 1, 2 * ways
    stats_of = (STATS, lambda to: stats, lambda s: stats_in.at[s])
    dots_of = (DOTS, lambda to: dots, lambda s: dots_in.at[s])

    loads = [
        pltpu.make_async_copy(src, dst, local_sem.at[k])
        for k, (src, dst) in enumerate(
            [
                (router_hbm, router), (tok_hbm, tok), (cot_hbm, cot),
                (w_in_hbm, w_in), (w_out_hbm, w_out),
            ]
        )
    ]
    for load in loads:
        load.start()

    barrier = pltpu.get_barrier_semaphore()

    for k in sorted(range(1, depth), key=lambda k: -min(k, depth - k)):
        pl.semaphore_signal(
            barrier, inc=1, device_id={"dp": lax.rem(me_z + k, depth) * PLANE + me_q},
            device_id_type=MESH,
        )
    for q, t in near:
        pl.semaphore_signal(
            barrier, inc=1, device_id={"dp": me_z * PLANE + q, "tensor": t}, device_id_type=MESH
        )

    def belongs(slot, at):
        e = lax.rem(slot, own)
        first = e * half + (slot - e) * (images // own)
        return (at >= first) & (at < first + images)

    row, col = iotas((c, slots))
    choose = jnp.where(belongs(col, row), 1.0, 0.0).astype(LOW)
    loads[0].wait()
    spread[...] = plain(choose, router[...]).astype(LOW)
    loads[1].wait()
    row, col = iotas((c, n))
    begin = lax.rem(row, images) * seq
    ours = (col >= begin) & (col < begin + seq)
    masked = jnp.where(ours, rows_by_rows(spread[...], tok[...]), LEAST)
    top = jnp.max(masked, axis=1, keepdims=True)
    exponent = jnp.where(ours, jnp.exp(masked - top), 0.0)
    exponent_low = exponent.astype(LOW)
    weight[...] = exponent
    lane = iotas((c, LANES))[1]
    packed = jnp.where(
        lane == 0, top,
        jnp.where(
            lane == 1, jnp.sum(exponent, axis=1, keepdims=True),
            jnp.sum(exponent_low.astype(WIDE), axis=1, keepdims=True),
        ),
    )
    stats[...] = jnp.transpose(packed)[0:8, :]

    across = depth * images

    def cut(rows, lot):
        k = number[lot]
        for t in range(tp):
            block = rows[:, t * LANES:(t + 1) * LANES]
            if lot[0] == 0:
                out_send[k, t] = block.reshape(dp, images, LANES).astype(LOW)
            else:
                for q in range(PLANE):
                    share = block[q * across:(q + 1) * across].reshape(depth, images, LANES)
                    back_send[k - ways, q * tp + t] = share.astype(LOW)

    def begin_sum(rows, lot):
        cut(rows, lot)
        if lot[0] == 0:
            start_tensor(*tensor_of[number[lot]])
        else:
            start_plane(*plane_of[number[lot]])

    cut(plain(exponent_low[0:half], tok[...]), (0, 0, 0))
    pl.semaphore_wait(barrier, members + depth - 2)
    start_tensor(*stats_of)
    start_tensor(*tensor_of[0])
    for e in range(1, own):
        begin_sum(plain(exponent_low[e * half:(e + 1) * half], tok[...]), (0, 0, e))

    loads[2].wait()
    best = jnp.max(masked, axis=0, keepdims=True)
    raised = jnp.where(ours, jnp.exp(masked - best), 0.0)
    share = raised / jnp.sum(raised, axis=0, keepdims=True)
    combine[...] = share
    share_low = share.astype(LOW)
    for e in range(own):
        begin_sum(plain(share_low[e * half:(e + 1) * half], cot[...]), (0, 1, e))

    await_tensor(*stats_of)
    stats_in[me_t] = stats[...]
    most = stats_in[0, 0:1]
    for s in range(1, tp):
        most = jnp.maximum(most, stats_in[s, 0:1])
    shrinks = [jnp.exp(stats_in[s, 0:1] - most) for s in range(tp)]
    total = sum(stats_in[s, 1:2] * shrinks[s] for s in range(tp))
    total_low = sum(stats_in[s, 2:3] * shrinks[s] for s in range(tp))
    lines = [
        jnp.exp((stats_in[before(k), 0:1] if k else stats[0:1]) - most) / total_low
        for k in range(tp)
    ]
    lines.append(jnp.exp(stats[0:1] - most) / total)
    line_row = iotas((LANES, c))[0]
    table = jnp.zeros((LANES, c), WIDE)
    for s, line in enumerate(lines):
        table = jnp.where(line_row == s, line, table)
    table = jnp.transpose(table)
    dispatch[...] = weight[...] * table[:, tp:tp + 1]

    def pass_on(lot):
        k, e = number[lot], lot[2]
        if lot[0] == 0:
            total_rows = None
            for back in range(tp):
                if back:
                    await_one(back, *tensor_of[k])
                    term = out_recv[k, before(back)]
                else:
                    term = out_send[k, me_t]
                term = term.astype(WIDE).reshape(half, LANES)
                if lot[1] == 0:
                    term = term * table[e * half:(e + 1) * half, back:back + 1]
                total_rows = term if total_rows is None else total_rows + term
            if lot[1] == 0:
                slot_slice[e * half:(e + 1) * half] = total_rows
            send_slots[k] = total_rows.reshape(depth, PLANE, images, LANES).astype(LOW)
        else:
            all_plane(k, back_recv.at[k - ways]).wait_recv()
            back_recv[k - ways, me_p] = back_send[k - ways, me_p]
            for q in range(PLANE):
                total_rows = back_recv[k - ways, q * tp].astype(WIDE)
                for t in range(1, tp):
                    total_rows = total_rows + back_recv[k - ways, q * tp + t].astype(WIDE)
                send_slots[k, :, q] = total_rows.astype(LOW)
        start_z(*z_of[k])

    def gather(lot):
        k = number[lot]
        await_z(*z_of[k])
        if lot[0] == 0:
            slots_out[k, :, me_z] = send_slots[k, me_z]
            start_plane(*plane_of[k])
        else:
            slots_back[k - ways, me_z] = send_slots[k, me_z]
            start_tensor(*tensor_of[k])

    def assembled(lot):
        k, (turn, kind, e) = number[lot], lot
        if turn == 0:
            all_plane(k, full_out.at[k]).wait_recv()
            full_out[k, me_p] = slots_out[k, me_q]
            for q in range(PLANE):
                rows = slice(e * half + q * across, e * half + (q + 1) * across)
                for t in range(tp):
                    block = full_out[k, q * tp + t].astype(WIDE).reshape(across, LANES)
                    flat[turn, kind, rows, t * LANES:(t + 1) * LANES] = block.astype(LOW)
        else:
            await_tensor(*tensor_of[k])
            full_back[k - ways, me_t] = slots_back[k - ways]
            for t in range(tp):
                block = full_back[k - ways, t].astype(WIDE).reshape(half, LANES)
                flat[turn, kind, e * half:(e + 1) * half, t * LANES:(t + 1) * LANES] = (
                    block.astype(LOW)
                )
        return flat[turn, kind, e * half:(e + 1) * half]

    root = math.sqrt(2.0 / math.pi)
    slope = {}

    def expert_out(e):
        pre = plain(assembled((0, 0, e)), w_in[e])
        square = pre * pre
        bent = jnp.tanh(root * (pre + 0.044715 * (square * pre)))
        hidden[e] = (0.5 * pre * (1.0 + bent)).astype(LOW)
        slope[e] = 0.5 * (1.0 + bent) + 0.5 * pre * (1.0 - bent * bent) * (
            root * (1.0 + 3.0 * 0.044715 * square)
        )
        begin_sum(plain(hidden[e], w_out[e]), (1, 0, e))

    def expert_back(e):
        grad_hidden = rows_by_rows(assembled((0, 1, e)), w_out[e])
        grad_pre[e] = (slope[e] * grad_hidden).astype(LOW)
        begin_sum(rows_by_rows(grad_pre[e], w_in[e]), (1, 1, e))

    pass_on((0, 0, 0))
    pass_on((0, 0, 1))
    pass_on((0, 1, 0))
    gather((0, 0, 0))
    pass_on((0, 1, 1))
    gather((0, 0, 1))
    gather((0, 1, 0))
    for load in loads[3:]:
        load.wait()
    gather((0, 1, 1))
    expert_out(0)
    expert_out(1)
    expert_back(0)
    expert_back(1)
    pass_on((1, 0, 0))
    pass_on((1, 0, 1))
    pass_on((1, 1, 0))
    gather((1, 0, 0))
    pass_on((1, 1, 1))
    gather((1, 0, 1))
    gather((1, 1, 0))
    gather((1, 1, 1))
    products = jnp.concatenate([
        slots_back[number[(1, 1, e)] - ways].astype(WIDE).reshape(half, LANES) for e in range(own)
    ]) * slot_slice[...]
    own_dots = jnp.broadcast_to(jnp.sum(products, axis=1, keepdims=True), (c, LANES))
    dots[...] = jnp.transpose(own_dots)[0:8, :]
    start_tensor(*dots_of)
    for e in range(own):
        here = slice(e * half, (e + 1) * half)
        grad_out[e] = columns_by_columns(hidden[e], flat[0, 1, here]).astype(LOW)
        grad_in[e] = columns_by_columns(flat[0, 0, here], grad_pre[e]).astype(LOW)

    share = combine[...]
    grad_share = jnp.concatenate(
        [rows_by_rows(assembled((1, 0, e)), cot[...]) for e in range(own)]
    )
    row_dot = jnp.sum(grad_share * share, axis=0, keepdims=True)
    from_share = share * (grad_share - row_dot)
    grad_weight = jnp.concatenate(
        [rows_by_rows(assembled((1, 1, e)), tok[...]) for e in range(own)]
    )
    slot_grad = flat[1, 1]
    await_tensor(*dots_of)
    dots_in[me_t] = dots[...]
    dot_line = dots_in[0, 0:1]
    for s in range(1, tp):
        dot_line = dot_line + dots_in[s, 0:1]
    column_dot = jnp.transpose(jnp.broadcast_to(dot_line, (LANES, c)))[:, 0:1]
    spots = dispatch[...]
    grad_logits = (from_share + spots * (grad_weight - column_dot)).astype(LOW)
    row, col = iotas((slots, c))
    fold = jnp.where(belongs(row, col), 1.0, 0.0).astype(LOW)
    by_slot = plain(fold, grad_logits).astype(LOW)
    local_router = plain(by_slot, tok[...])
    high = slots // PLANE
    for q in range(PLANE):
        for t in range(tp):
            part[q * tp + t] = local_router[
                q * high:(q + 1) * high, t * LANES:(t + 1) * LANES
            ].astype(LOW)

    start_plane(PART, lambda q, t: part.at[q * tp + t], part_in.at[me_p])
    grad_tok[...] = (
        columns_by_columns(spots.astype(LOW), slot_grad)
        + columns_by_columns(grad_logits, spread[...])
    ).astype(LOW)

    all_plane(PART, part_in).wait_recv()
    part_in[me_p] = part[me_p]
    piece[...] = jnp.sum(part_in[...].astype(WIDE), axis=0)
    piece_of = (PIECE, lambda to: piece, lambda s: piece_in.at[s])
    start_z(*piece_of)
    await_z(*piece_of)
    piece_in[me_z] = piece[...]
    final[...] = jnp.sum(piece_in[...], axis=0).astype(LOW)
    start_plane(WHOLE, lambda q, t: final, whole.at[me_p])
    all_plane(WHOLE, whole).wait_recv()
    whole[me_p] = final[...]
    for q in range(PLANE):
        for t in range(tp):
            grad_router[q * high:(q + 1) * high, t * LANES:(t + 1) * LANES] = (
                whole[q * tp + t].astype(WIDE)
            )

    for phase in [*tensor_of, stats_of, dots_of]:
        drain_tensor(*phase)
    for phase in [*z_of, piece_of]:
        drain_z(*phase)
    for k in range(ways):
        all_plane(k, full_out.at[k]).wait_send()
        all_plane(ways + k, back_recv.at[k]).wait_send()
    all_plane(PART, part_in).wait_send()
    all_plane(WHOLE, whole).wait_send()


def finish(*refs):
    count = (len(refs) - 1) // 2
    copies = [
        pltpu.make_async_copy(refs[k], refs[count + k], refs[-1].at[k]) for k in range(count)
    ]
    for copy in copies:
        copy.start()
    for copy in copies:
        copy.wait()


def on_device(tokens, cotangent, dispatch_weight, w_in, w_out):
    tp, dp = lax.axis_size("tensor"), lax.axis_size("dp")
    images, seq, width = tokens.shape
    own, _, inner = w_in.shape
    n, slots, group = images * seq, dp * own, own * images
    c = dp * group
    members, depth, high, ways = PLANE * tp, dp // PLANE, slots // PLANE, 2 * own
    vmem, hbm = pltpu.VMEM, pl.BlockSpec(memory_space=pltpu.HBM)
    here = pl.BlockSpec(memory_space=pltpu.VMEM)
    shapes = [((n, width), LOW), ((slots, width), WIDE), (w_in.shape, LOW), (w_out.shape, LOW)]
    outs = pl.pallas_call(
        functools.partial(kernel, tp, dp, images, own),
        name="moe_back",
        out_shape=tuple(vmem(*shape) for shape in shapes),
        in_specs=[hbm] * 5,
        out_specs=(here,) * 4,
        scratch_shapes=[
            vmem((slots, width), LOW), vmem((n, width), LOW), vmem((n, width), LOW),
            vmem(w_in.shape, LOW), vmem(w_out.shape, LOW),
            vmem((c, width), LOW),
            vmem((c, n), WIDE), vmem((c, n), WIDE), vmem((c, n), WIDE),
            vmem((c, LANES), WIDE),
            vmem((ways, tp, dp, images, LANES), LOW), vmem((ways, tp, dp, images, LANES), LOW),
            vmem((ways, members, depth, images, LANES), LOW),
            vmem((ways, members, depth, images, LANES), LOW),
            vmem((2 * ways, depth, PLANE, images, LANES), LOW),
            vmem((ways, PLANE, depth, images, LANES), LOW),
            vmem((ways, depth, PLANE, images, LANES), LOW),
            vmem((ways, members, depth, images, LANES), LOW),
            vmem((ways, tp, depth, PLANE, images, LANES), LOW),
            vmem((2, 2, c, width), LOW),
            vmem((own, c // own, inner), LOW), vmem((own, c // own, inner), LOW),
            vmem((8, c), WIDE), vmem((tp, 8, c), WIDE),
            vmem((8, c), WIDE), vmem((tp, 8, c), WIDE),
            vmem((members, high, LANES), LOW), vmem((members, high, LANES), LOW),
            vmem((high, LANES), WIDE), vmem((depth, high, LANES), WIDE),
            vmem((members, high, LANES), LOW), vmem((high, LANES), LOW),
            pltpu.SemaphoreType.DMA((5,)),
            pltpu.SemaphoreType.DMA((2 * ways + 2, tp)), pltpu.SemaphoreType.DMA((2 * ways + 2, tp)),
            pltpu.SemaphoreType.DMA((2 * ways + 2,)), pltpu.SemaphoreType.DMA((2 * ways + 2,)),
            pltpu.SemaphoreType.DMA((2 * ways + 1, depth)),
            pltpu.SemaphoreType.DMA((2 * ways + 1, depth)),
        ],
        compiler_params=pltpu.CompilerParams(
            collective_id=0, has_side_effects=True, vmem_limit_bytes=61400000
        ),
    )(
        dispatch_weight.T, tokens.reshape(n, width), cotangent.reshape(n, width), w_in, w_out
    )
    grad_tokens, grad_router, grad_w_in, grad_w_out = pl.pallas_call(
        finish,
        name="finish",
        out_shape=tuple(jax.ShapeDtypeStruct(*shape) for shape in shapes),
        in_specs=[here] * 4,
        out_specs=(hbm,) * 4,
        scratch_shapes=[pltpu.SemaphoreType.DMA((4,))],
        compiler_params=pltpu.CompilerParams(vmem_limit_bytes=4 * 2**20),
    )(*outs)
    return (grad_tokens.reshape(tokens.shape), grad_router.T, grad_w_in, grad_w_out)


def solution(mesh):
    return jax.shard_map(
        on_device,
        mesh=mesh,
        in_specs=(
            P("dp", "tensor", None),
            P("dp", "tensor", None),
            P(),
            P("dp", None, "tensor"),
            P("dp", "tensor", None),
        ),
        out_specs=(P("dp", "tensor", None), P(), P("dp", None, "tensor"), P("dp", "tensor", None)),
        check_vma=False,
    )
```

```python
import functools
import math

import jax
import jax.numpy as jnp
from jax import lax
from jax.experimental import pallas as pl
from jax.experimental.pallas import tpu as pltpu
from jax.sharding import PartitionSpec as P

WIDE = jnp.float32
LOW = jnp.bfloat16
MESH = pl.DeviceIdType.MESH
LANES = 128
LEAST = -3.0e38
PLANE = 4


def dot(a, b, over):
    return lax.dot_general(a, b, (over, ((), ())), preferred_element_type=WIDE)


def plain(a, b):
    return dot(a, b, ((1,), (0,)))


def rows_by_rows(a, b):
    return dot(a, b, ((1,), (1,)))


def columns_by_columns(a, b):
    return dot(a, b, ((0,), (0,)))


def iotas(shape):
    return lax.broadcasted_iota(jnp.int32, shape, 0), lax.broadcasted_iota(jnp.int32, shape, 1)


def kernel(
    tp, dp, images, own,
    router_hbm, tok_hbm, cot_hbm, w_in_hbm, w_out_hbm,
    grad_tok, grad_router, grad_in, grad_out,
    router, tok, cot, w_in, w_out, spread, weight, combine, dispatch, slot_slice,
    out_send, out_recv, back_send, back_recv, send_slots, slots_out, slots_back,
    full_out, full_back, flat, hidden, grad_pre,
    stats, stats_in,
    dots, dots_in, part, part_in, piece, piece_in, whole, final,
    local_sem, t_send, t_recv, p_send, p_recv, z_send, z_recv,
):
    me_t, me_d = lax.axis_index("tensor"), lax.axis_index("dp")
    n = tok.shape[0]
    group = own * images
    c = dp * group
    seq = n // images
    slots = dp * own
    half = c // own
    members, depth = PLANE * tp, dp // PLANE
    me_z, me_q = me_d // PLANE, lax.rem(me_d, PLANE)
    me_p = me_q * tp + me_t

    def remote(src, dst, send_sem, recv_sem, where):
        return pltpu.make_async_remote_copy(
            src_ref=src, dst_ref=dst, send_sem=send_sem, recv_sem=recv_sem,
            device_id=where, device_id_type=MESH,
        )

    def outward(size):
        return sorted(range(1, size), key=lambda k: -min(k, size - k))

    def start_tensor(phase, src, dst, bulk):
        for k in outward(tp):
            to = lax.rem(me_t + k, tp)
            remote(
                src(to), dst, t_send.at[phase], t_recv.at[phase], {"tensor": to}
            ).start()

    def all_tensor(phase, src, dst, bulk):
        return remote(
            bulk, bulk, t_send.at[phase], t_recv.at[phase], {"tensor": lax.rem(me_t + 1, tp)}
        )

    def before(k):
        return lax.rem(me_t + tp - k, tp)

    near = [
        (lax.rem(me_q + jq, PLANE), lax.rem(me_t + jt, tp))
        for jt in sorted(range(tp), key=lambda jt: -min(jt, tp - jt))
        for jq in sorted(range(PLANE), key=lambda jq: -min(jq, PLANE - jq))
        if (jq, jt) != (0, 0)
    ]

    def start_plane(phase, src, dst):
        for q, t in near:
            remote(
                src(q, t), dst, p_send.at[phase], p_recv.at[phase],
                {"dp": me_z * PLANE + q, "tensor": t},
            ).start()

    def all_plane(phase, blocks):
        few = blocks.at[pl.ds(0, members - 1)]
        q, t = near[0]
        return remote(
            few, few, p_send.at[phase], p_recv.at[phase], {"dp": me_z * PLANE + q, "tensor": t}
        )

    def start_z(phase, src, dst, bulk):
        for k in outward(depth):
            to = lax.rem(me_z + k, depth)
            remote(
                src(to), dst, z_send.at[phase], z_recv.at[phase], {"dp": to * PLANE + me_q}
            ).start()

    def all_z(phase, src, dst, bulk):
        to = lax.rem(me_z + 1, depth)
        return remote(
            bulk, bulk, z_send.at[phase], z_recv.at[phase], {"dp": to * PLANE + me_q}
        )

    lots = [(turn, kind, e) for turn in range(2) for kind in range(2) for e in range(own)]
    number = {lot: k for k, lot in enumerate(lots)}
    STATS, DOTS = len(lots), len(lots) + 1
    ways = len(lots) // 2
    few_t, few_z = pl.ds(0, tp - 1), pl.ds(0, depth - 1)
    tensor_of = [
        (k, lambda to, k=k: out_send.at[k, to], out_recv.at[k, me_t], out_recv.at[k, few_t])
        for k in range(ways)
    ] + [
        (
            ways + k, lambda to, k=k: slots_back.at[k], full_back.at[k, me_t],
            full_back.at[k, few_t],
        )
        for k in range(ways)
    ]
    plane_of = [
        (k, lambda q, t, k=k: slots_out.at[k, q], full_out.at[k, me_p]) for k in range(ways)
    ] + [
        (ways + k, lambda q, t, k=k: back_send.at[k, q * tp + t], back_recv.at[k, me_p])
        for k in range(ways)
    ]
    z_of = [
        (
            k, lambda to, k=k: send_slots.at[k, to], slots_out.at[k, :, me_z],
            send_slots.at[k, few_z],
        )
        for k in range(ways)
    ] + [
        (
            ways + k, lambda to, k=k: send_slots.at[ways + k, to], slots_back.at[k, me_z],
            slots_back.at[k, few_z],
        )
        for k in range(ways)
    ]
    PART, WHOLE, PIECE = 2 * ways, 2 * ways + 1, 2 * ways
    stats_of = (STATS, lambda to: stats, stats_in.at[me_t], stats_in.at[few_t])
    dots_of = (DOTS, lambda to: dots, dots_in.at[me_t], dots_in.at[few_t])

    loads = [
        pltpu.make_async_copy(src, dst, local_sem.at[k])
        for k, (src, dst) in enumerate(
            [
                (router_hbm, router), (tok_hbm, tok), (cot_hbm, cot),
                (w_in_hbm, w_in), (w_out_hbm, w_out),
            ]
        )
    ]
    for load in loads:
        load.start()

    barrier = pltpu.get_barrier_semaphore()

    for k in outward(depth):
        pl.semaphore_signal(
            barrier, inc=1, device_id={"dp": lax.rem(me_z + k, depth) * PLANE + me_q},
            device_id_type=MESH,
        )
    for q, t in near:
        pl.semaphore_signal(
            barrier, inc=1, device_id={"dp": me_z * PLANE + q, "tensor": t}, device_id_type=MESH
        )

    def belongs(slot, at):
        e = lax.rem(slot, own)
        first = e * half + (slot - e) * (images // own)
        return (at >= first) & (at < first + images)

    row, col = iotas((c, slots))
    choose = jnp.where(belongs(col, row), 1.0, 0.0).astype(LOW)
    loads[0].wait()
    spread[...] = plain(choose, router[...]).astype(LOW)
    loads[1].wait()
    row, col = iotas((c, n))
    begin = lax.rem(row, images) * seq
    ours = (col >= begin) & (col < begin + seq)
    masked = jnp.where(ours, rows_by_rows(spread[...], tok[...]), LEAST)
    top = jnp.max(masked, axis=1, keepdims=True)
    exponent = jnp.where(ours, jnp.exp(masked - top), 0.0)
    exponent_low = exponent.astype(LOW)
    weight[...] = exponent
    lane = iotas((c, LANES))[1]
    packed = jnp.where(
        lane == 0, top,
        jnp.where(
            lane == 1, jnp.sum(exponent, axis=1, keepdims=True),
            jnp.sum(exponent_low.astype(WIDE), axis=1, keepdims=True),
        ),
    )
    stats[...] = jnp.transpose(packed)[0:8, :]

    across = depth * images

    def cut(rows, lot):
        k = number[lot]
        for t in range(tp):
            block = rows[:, t * LANES:(t + 1) * LANES]
            if lot[0] == 0:
                out_send[k, t] = block.reshape(dp, images, LANES).astype(LOW)
            else:
                for q in range(PLANE):
                    share = block[q * across:(q + 1) * across].reshape(depth, images, LANES)
                    back_send[k - ways, q * tp + t] = share.astype(LOW)

    def begin_sum(rows, lot):
        cut(rows, lot)
        if lot[0] == 0:
            start_tensor(*tensor_of[number[lot]])
        else:
            start_plane(*plane_of[number[lot]])

    cut(plain(exponent_low[0:half], tok[...]), (0, 0, 0))
    pl.semaphore_wait(barrier, members + depth - 2)
    start_tensor(*stats_of)
    start_tensor(*tensor_of[0])
    for e in range(1, own):
        begin_sum(plain(exponent_low[e * half:(e + 1) * half], tok[...]), (0, 0, e))

    loads[2].wait()
    best = jnp.max(masked, axis=0, keepdims=True)
    raised = jnp.where(ours, jnp.exp(masked - best), 0.0)
    share = raised / jnp.sum(raised, axis=0, keepdims=True)
    combine[...] = share
    share_low = share.astype(LOW)
    for e in range(own):
        begin_sum(plain(share_low[e * half:(e + 1) * half], cot[...]), (0, 1, e))

    all_tensor(*stats_of).wait_recv()
    stats_in[me_t] = stats[...]
    most = stats_in[0, 0:1]
    for s in range(1, tp):
        most = jnp.maximum(most, stats_in[s, 0:1])
    shrinks = [jnp.exp(stats_in[s, 0:1] - most) for s in range(tp)]
    total = sum(stats_in[s, 1:2] * shrinks[s] for s in range(tp))
    total_low = sum(stats_in[s, 2:3] * shrinks[s] for s in range(tp))
    lines = [
        jnp.exp((stats_in[before(k), 0:1] if k else stats[0:1]) - most) / total_low
        for k in range(tp)
    ]
    lines.append(jnp.exp(stats[0:1] - most) / total)
    line_row = iotas((LANES, c))[0]
    table = jnp.zeros((LANES, c), WIDE)
    for s, line in enumerate(lines):
        table = jnp.where(line_row == s, line, table)
    table = jnp.transpose(table)
    dispatch[...] = weight[...] * table[:, tp:tp + 1]

    def pass_on(lot):
        k, e = number[lot], lot[2]
        if lot[0] == 0:
            all_tensor(*tensor_of[k]).wait_recv()
            total_rows = None
            for back in range(tp):
                if back:
                    term = out_recv[k, before(back)]
                else:
                    term = out_send[k, me_t]
                term = term.astype(WIDE).reshape(half, LANES)
                if lot[1] == 0:
                    term = term * table[e * half:(e + 1) * half, back:back + 1]
                total_rows = term if total_rows is None else total_rows + term
            if lot[1] == 0:
                slot_slice[e * half:(e + 1) * half] = total_rows
            send_slots[k] = total_rows.reshape(depth, PLANE, images, LANES).astype(LOW)
        else:
            all_plane(k, back_recv.at[k - ways]).wait_recv()
            back_recv[k - ways, me_p] = back_send[k - ways, me_p]
            for q in range(PLANE):
                total_rows = back_recv[k - ways, q * tp].astype(WIDE)
                for t in range(1, tp):
                    total_rows = total_rows + back_recv[k - ways, q * tp + t].astype(WIDE)
                send_slots[k, :, q] = total_rows.astype(LOW)
        start_z(*z_of[k])

    def gather(lot):
        k = number[lot]
        all_z(*z_of[k]).wait_recv()
        if lot[0] == 0:
            slots_out[k, :, me_z] = send_slots[k, me_z]
            start_plane(*plane_of[k])
        else:
            slots_back[k - ways, me_z] = send_slots[k, me_z]
            start_tensor(*tensor_of[k])

    def assembled(lot):
        k, (turn, kind, e) = number[lot], lot
        if turn == 0:
            all_plane(k, full_out.at[k]).wait_recv()
            full_out[k, me_p] = slots_out[k, me_q]
            for q in range(PLANE):
                rows = slice(e * half + q * across, e * half + (q + 1) * across)
                for t in range(tp):
                    block = full_out[k, q * tp + t].astype(WIDE).reshape(across, LANES)
                    flat[turn, kind, rows, t * LANES:(t + 1) * LANES] = block.astype(LOW)
        else:
            all_tensor(*tensor_of[k]).wait_recv()
            full_back[k - ways, me_t] = slots_back[k - ways]
            for t in range(tp):
                block = full_back[k - ways, t].astype(WIDE).reshape(half, LANES)
                flat[turn, kind, e * half:(e + 1) * half, t * LANES:(t + 1) * LANES] = (
                    block.astype(LOW)
                )
        return flat[turn, kind, e * half:(e + 1) * half]

    root = math.sqrt(2.0 / math.pi)
    slope = {}

    def expert_out(e):
        pre = plain(assembled((0, 0, e)), w_in[e])
        square = pre * pre
        bent = jnp.tanh(root * (pre + 0.044715 * (square * pre)))
        hidden[e] = (0.5 * pre * (1.0 + bent)).astype(LOW)
        slope[e] = 0.5 * (1.0 + bent) + 0.5 * pre * (1.0 - bent * bent) * (
            root * (1.0 + 3.0 * 0.044715 * square)
        )
        begin_sum(plain(hidden[e], w_out[e]), (1, 0, e))

    def expert_back(e):
        grad_hidden = rows_by_rows(assembled((0, 1, e)), w_out[e])
        grad_pre[e] = (slope[e] * grad_hidden).astype(LOW)
        begin_sum(rows_by_rows(grad_pre[e], w_in[e]), (1, 1, e))

    pass_on((0, 0, 0))
    pass_on((0, 0, 1))
    pass_on((0, 1, 0))
    gather((0, 0, 0))
    pass_on((0, 1, 1))
    gather((0, 0, 1))
    gather((0, 1, 0))
    for load in loads[3:]:
        load.wait()
    gather((0, 1, 1))
    expert_out(0)
    expert_out(1)
    expert_back(0)
    expert_back(1)
    pass_on((1, 0, 0))
    pass_on((1, 0, 1))
    pass_on((1, 1, 0))
    gather((1, 0, 0))
    pass_on((1, 1, 1))
    gather((1, 0, 1))
    gather((1, 1, 0))
    gather((1, 1, 1))
    products = jnp.concatenate([
        slots_back[number[(1, 1, e)] - ways].astype(WIDE).reshape(half, LANES) for e in range(own)
    ]) * slot_slice[...]
    own_dots = jnp.broadcast_to(jnp.sum(products, axis=1, keepdims=True), (c, LANES))
    dots[...] = jnp.transpose(own_dots)[0:8, :]
    start_tensor(*dots_of)
    for e in range(own):
        here = slice(e * half, (e + 1) * half)
        grad_out[e] = columns_by_columns(hidden[e], flat[0, 1, here]).astype(LOW)
        grad_in[e] = columns_by_columns(flat[0, 0, here], grad_pre[e]).astype(LOW)

    share = combine[...]
    grad_share = jnp.concatenate(
        [rows_by_rows(assembled((1, 0, e)), cot[...]) for e in range(own)]
    )
    row_dot = jnp.sum(grad_share * share, axis=0, keepdims=True)
    from_share = share * (grad_share - row_dot)
    grad_weight = jnp.concatenate(
        [rows_by_rows(assembled((1, 1, e)), tok[...]) for e in range(own)]
    )
    slot_grad = flat[1, 1]
    all_tensor(*dots_of).wait_recv()
    dots_in[me_t] = dots[...]
    dot_line = dots_in[0, 0:1]
    for s in range(1, tp):
        dot_line = dot_line + dots_in[s, 0:1]
    column_dot = jnp.transpose(jnp.broadcast_to(dot_line, (LANES, c)))[:, 0:1]
    spots = dispatch[...]
    grad_logits = (from_share + spots * (grad_weight - column_dot)).astype(LOW)
    row, col = iotas((slots, c))
    fold = jnp.where(belongs(row, col), 1.0, 0.0).astype(LOW)
    by_slot = plain(fold, grad_logits).astype(LOW)
    local_router = plain(by_slot, tok[...])
    high = slots // PLANE
    for q in range(PLANE):
        for t in range(tp):
            part[q * tp + t] = local_router[
                q * high:(q + 1) * high, t * LANES:(t + 1) * LANES
            ].astype(LOW)

    start_plane(PART, lambda q, t: part.at[q * tp + t], part_in.at[me_p])
    grad_tok[...] = (
        columns_by_columns(spots.astype(LOW), slot_grad)
        + columns_by_columns(grad_logits, spread[...])
    ).astype(LOW)

    all_plane(PART, part_in).wait_recv()
    part_in[me_p] = part[me_p]
    piece[...] = jnp.sum(part_in[...].astype(WIDE), axis=0)
    piece_of = (PIECE, lambda to: piece, piece_in.at[me_z], piece_in.at[few_z])
    start_z(*piece_of)
    all_z(*piece_of).wait_recv()
    piece_in[me_z] = piece[...]
    final[...] = jnp.sum(piece_in[...], axis=0).astype(LOW)
    start_plane(WHOLE, lambda q, t: final, whole.at[me_p])
    all_plane(WHOLE, whole).wait_recv()
    whole[me_p] = final[...]
    for q in range(PLANE):
        for t in range(tp):
            grad_router[q * high:(q + 1) * high, t * LANES:(t + 1) * LANES] = (
                whole[q * tp + t].astype(WIDE)
            )

    for phase in [*tensor_of, stats_of, dots_of]:
        all_tensor(*phase).wait_send()
    for phase in [*z_of, piece_of]:
        all_z(*phase).wait_send()
    for k in range(ways):
        all_plane(k, full_out.at[k]).wait_send()
        all_plane(ways + k, back_recv.at[k]).wait_send()
    all_plane(PART, part_in).wait_send()
    all_plane(WHOLE, whole).wait_send()


def finish(*refs):
    count = (len(refs) - 1) // 2
    copies = [
        pltpu.make_async_copy(refs[k], refs[count + k], refs[-1].at[k]) for k in range(count)
    ]
    for copy in copies:
        copy.start()
    for copy in copies:
        copy.wait()


def on_device(tokens, cotangent, dispatch_weight, w_in, w_out):
    tp, dp = lax.axis_size("tensor"), lax.axis_size("dp")
    images, seq, width = tokens.shape
    own, _, inner = w_in.shape
    n, slots, group = images * seq, dp * own, own * images
    c = dp * group
    members, depth, high, ways = PLANE * tp, dp // PLANE, slots // PLANE, 2 * own
    vmem, hbm = pltpu.VMEM, pl.BlockSpec(memory_space=pltpu.HBM)
    here = pl.BlockSpec(memory_space=pltpu.VMEM)
    shapes = [((n, width), LOW), ((slots, width), WIDE), (w_in.shape, LOW), (w_out.shape, LOW)]
    outs = pl.pallas_call(
        functools.partial(kernel, tp, dp, images, own),
        name="moe_back",
        out_shape=tuple(vmem(*shape) for shape in shapes),
        in_specs=[hbm] * 5,
        out_specs=(here,) * 4,
        scratch_shapes=[
            vmem((slots, width), LOW), vmem((n, width), LOW), vmem((n, width), LOW),
            vmem(w_in.shape, LOW), vmem(w_out.shape, LOW),
            vmem((c, width), LOW),
            vmem((c, n), WIDE), vmem((c, n), WIDE), vmem((c, n), WIDE),
            vmem((c, LANES), WIDE),
            vmem((ways, tp, dp, images, LANES), LOW), vmem((ways, tp, dp, images, LANES), LOW),
            vmem((ways, members, depth, images, LANES), LOW),
            vmem((ways, members, depth, images, LANES), LOW),
            vmem((2 * ways, depth, PLANE, images, LANES), LOW),
            vmem((ways, PLANE, depth, images, LANES), LOW),
            vmem((ways, depth, PLANE, images, LANES), LOW),
            vmem((ways, members, depth, images, LANES), LOW),
            vmem((ways, tp, depth, PLANE, images, LANES), LOW),
            vmem((2, 2, c, width), LOW),
            vmem((own, c // own, inner), LOW), vmem((own, c // own, inner), LOW),
            vmem((8, c), WIDE), vmem((tp, 8, c), WIDE),
            vmem((8, c), WIDE), vmem((tp, 8, c), WIDE),
            vmem((members, high, LANES), LOW), vmem((members, high, LANES), LOW),
            vmem((high, LANES), WIDE), vmem((depth, high, LANES), WIDE),
            vmem((members, high, LANES), LOW), vmem((high, LANES), LOW),
            pltpu.SemaphoreType.DMA((5,)),
            pltpu.SemaphoreType.DMA((2 * ways + 2,)), pltpu.SemaphoreType.DMA((2 * ways + 2,)),
            pltpu.SemaphoreType.DMA((2 * ways + 2,)), pltpu.SemaphoreType.DMA((2 * ways + 2,)),
            pltpu.SemaphoreType.DMA((2 * ways + 1,)), pltpu.SemaphoreType.DMA((2 * ways + 1,)),
        ],
        compiler_params=pltpu.CompilerParams(
            collective_id=0, has_side_effects=True, vmem_limit_bytes=61400000
        ),
    )(
        dispatch_weight.T, tokens.reshape(n, width), cotangent.reshape(n, width), w_in, w_out
    )
    grad_tokens, grad_router, grad_w_in, grad_w_out = pl.pallas_call(
        finish,
        name="finish",
        out_shape=tuple(jax.ShapeDtypeStruct(*shape) for shape in shapes),
        in_specs=[here] * 4,
        out_specs=(hbm,) * 4,
        scratch_shapes=[pltpu.SemaphoreType.DMA((4,))],
        compiler_params=pltpu.CompilerParams(vmem_limit_bytes=4 * 2**20),
    )(*outs)
    return (grad_tokens.reshape(tokens.shape), grad_router.T, grad_w_in, grad_w_out)


def solution(mesh):
    return jax.shard_map(
        on_device,
        mesh=mesh,
        in_specs=(
            P("dp", "tensor", None),
            P("dp", "tensor", None),
            P(),
            P("dp", None, "tensor"),
            P("dp", "tensor", None),
        ),
        out_specs=(P("dp", "tensor", None), P(), P("dp", None, "tensor"), P("dp", "tensor", None)),
        check_vma=False,
    )
```

```python
import functools
import math

import jax
import jax.numpy as jnp
from jax import lax
from jax.experimental import pallas as pl
from jax.experimental.pallas import tpu as pltpu
from jax.sharding import PartitionSpec as P

WIDE = jnp.float32
LOW = jnp.bfloat16
MESH = pl.DeviceIdType.MESH
LANES = 128
LEAST = -3.0e38
PLANE = 4


def dot(a, b, over):
    return lax.dot_general(a, b, (over, ((), ())), preferred_element_type=WIDE)


def plain(a, b):
    return dot(a, b, ((1,), (0,)))


def rows_by_rows(a, b):
    return dot(a, b, ((1,), (1,)))


def columns_by_columns(a, b):
    return dot(a, b, ((0,), (0,)))


def iotas(shape):
    return lax.broadcasted_iota(jnp.int32, shape, 0), lax.broadcasted_iota(jnp.int32, shape, 1)


def kernel(
    tp, dp, images, own,
    router_hbm, tok_hbm, cot_hbm, w_in_hbm, w_out_hbm,
    grad_tok, grad_router, grad_in, grad_out,
    router, tok, cot, w_in, w_out, spread, weight, combine, dispatch, slot_slice,
    out_send, out_recv, back_send, back_recv, send_slots, slots_out, slots_back,
    full_out, full_back, flat, hidden, grad_pre,
    stats, stats_in,
    dots, dots_in, part, part_in, piece, piece_in, whole, final,
    local_sem, t_send, t_recv, p_send, p_recv, z_send, z_recv,
):
    me_t, me_d = lax.axis_index("tensor"), lax.axis_index("dp")
    n = tok.shape[0]
    group = own * images
    c = dp * group
    seq = n // images
    slots = dp * own
    half = c // own
    members, depth = PLANE * tp, dp // PLANE
    me_z, me_q = me_d // PLANE, lax.rem(me_d, PLANE)
    me_p = me_q * tp + me_t

    def remote(src, dst, send_sem, recv_sem, where):
        return pltpu.make_async_remote_copy(
            src_ref=src, dst_ref=dst, send_sem=send_sem, recv_sem=recv_sem,
            device_id=where, device_id_type=MESH,
        )

    def sent(phase):
        return min(phase // (2 * own), 2) if phase <= 4 * own else 3

    def outward(size):
        return sorted(range(1, size), key=lambda k: -min(k, size - k))

    def start_tensor(phase, src, dst, bulk):
        for k in outward(tp):
            to = lax.rem(me_t + k, tp)
            remote(
                src(to), dst, t_send.at[sent(phase)], t_recv.at[phase], {"tensor": to}
            ).start()

    def all_tensor(phase, src, dst, bulk):
        return remote(
            bulk, bulk, t_send.at[sent(phase)], t_recv.at[phase], {"tensor": lax.rem(me_t + 1, tp)}
        )

    def before(k):
        return lax.rem(me_t + tp - k, tp)

    near = [
        (lax.rem(me_q + jq, PLANE), lax.rem(me_t + jt, tp))
        for jt in sorted(range(tp), key=lambda jt: -min(jt, tp - jt))
        for jq in sorted(range(PLANE), key=lambda jq: -min(jq, PLANE - jq))
        if (jq, jt) != (0, 0)
    ]

    def start_plane(phase, src, dst):
        for q, t in near:
            remote(
                src(q, t), dst, p_send.at[sent(phase)], p_recv.at[phase],
                {"dp": me_z * PLANE + q, "tensor": t},
            ).start()

    def all_plane(phase, blocks):
        few = blocks.at[pl.ds(0, members - 1)]
        q, t = near[0]
        return remote(
            few, few, p_send.at[sent(phase)], p_recv.at[phase], {"dp": me_z * PLANE + q, "tensor": t}
        )

    def start_z(phase, src, dst, bulk):
        for k in outward(depth):
            to = lax.rem(me_z + k, depth)
            remote(
                src(to), dst, z_send.at[phase // (4 * own)], z_recv.at[phase], {"dp": to * PLANE + me_q}
            ).start()

    def all_z(phase, src, dst, bulk):
        to = lax.rem(me_z + 1, depth)
        return remote(
            bulk, bulk, z_send.at[phase // (4 * own)], z_recv.at[phase], {"dp": to * PLANE + me_q}
        )

    lots = [(turn, kind, e) for turn in range(2) for kind in range(2) for e in range(own)]
    number = {lot: k for k, lot in enumerate(lots)}
    DOTS, STATS = len(lots), len(lots) + 1
    ways = len(lots) // 2
    few_t, few_z = pl.ds(0, tp - 1), pl.ds(0, depth - 1)
    tensor_of = [
        (k, lambda to, k=k: out_send.at[k, to], out_recv.at[k, me_t], out_recv.at[k, few_t])
        for k in range(ways)
    ] + [
        (
            ways + k, lambda to, k=k: slots_back.at[k], full_back.at[k, me_t],
            full_back.at[k, few_t],
        )
        for k in range(ways)
    ]
    plane_of = [
        (k, lambda q, t, k=k: slots_out.at[k, q], full_out.at[k, me_p]) for k in range(ways)
    ] + [
        (ways + k, lambda q, t, k=k: back_send.at[k, q * tp + t], back_recv.at[k, me_p])
        for k in range(ways)
    ]
    z_of = [
        (
            k, lambda to, k=k: send_slots.at[k, to], slots_out.at[k, :, me_z],
            send_slots.at[k, few_z],
        )
        for k in range(ways)
    ] + [
        (
            ways + k, lambda to, k=k: send_slots.at[ways + k, to], slots_back.at[k, me_z],
            slots_back.at[k, few_z],
        )
        for k in range(ways)
    ]
    PART, WHOLE, PIECE = 2 * ways, 2 * ways + 1, 2 * ways
    stats_of = [
        (STATS + e, lambda to, e=e: stats.at[e], stats_in.at[e, me_t], stats_in.at[e, few_t])
        for e in range(own)
    ]
    dots_of = (DOTS, lambda to: dots, dots_in.at[me_t], dots_in.at[few_t])

    loads = [
        pltpu.make_async_copy(src, dst, local_sem.at[k])
        for k, (src, dst) in enumerate(
            [
                (router_hbm, router),
                (tok_hbm, tok),
                (cot_hbm, cot), (w_in_hbm, w_in), (w_out_hbm, w_out),
            ]
        )
    ]
    for load in loads:
        load.start()

    barrier = pltpu.get_barrier_semaphore()

    for k in outward(depth):
        pl.semaphore_signal(
            barrier, inc=1, device_id={"dp": lax.rem(me_z + k, depth) * PLANE + me_q},
            device_id_type=MESH,
        )
    for q, t in near:
        pl.semaphore_signal(
            barrier, inc=1, device_id={"dp": me_z * PLANE + q, "tensor": t}, device_id_type=MESH
        )

    def belongs(slot, at):
        e = lax.rem(slot, own)
        first = e * half + (slot - e) * (images // own)
        return (at >= first) & (at < first + images)

    row, col = iotas((c, slots))
    choose = jnp.where(belongs(col, row), 1.0, 0.0).astype(LOW)
    loads[0].wait()
    spread[...] = plain(choose, router[...]).astype(LOW)
    loads[1].wait()
    across = depth * images

    def cut(rows, lot):
        k = number[lot]
        for t in range(tp):
            block = rows[:, t * LANES:(t + 1) * LANES]
            if lot[0] == 0:
                out_send[k, t] = block.reshape(dp, images, LANES).astype(LOW)
            else:
                for q in range(PLANE):
                    share = block[q * across:(q + 1) * across].reshape(depth, images, LANES)
                    back_send[k - ways, q * tp + t] = share.astype(LOW)

    def begin_sum(rows, lot):
        cut(rows, lot)
        if lot[0] == 0:
            start_tensor(*tensor_of[number[lot]])
        else:
            start_plane(*plane_of[number[lot]])

    row, col = iotas((half, n))
    begin = lax.rem(row, images) * seq
    ours = (col >= begin) & (col < begin + seq)
    lane = iotas((half, LANES))[1]
    masked = []
    for e in range(own):
        here = slice(e * half, (e + 1) * half)
        masked.append(jnp.where(ours, rows_by_rows(spread[here], tok[...]), LEAST))
        top = jnp.max(masked[e], axis=1, keepdims=True)
        exponent = jnp.where(ours, jnp.exp(masked[e] - top), 0.0)
        exponent_low = exponent.astype(LOW)
        weight[here] = exponent
        packed = jnp.where(
            lane == 0, top,
            jnp.where(
                lane == 1, jnp.sum(exponent, axis=1, keepdims=True),
                jnp.sum(exponent_low.astype(WIDE), axis=1, keepdims=True),
            ),
        )
        stats[e] = jnp.transpose(packed)[0:8, :]
        cut(plain(exponent_low, tok[...]), (0, 0, e))
        if e == 0:
            pl.semaphore_wait(barrier, members + depth - 2)
        start_tensor(*stats_of[e])
        start_tensor(*tensor_of[e])

    loads[2].wait()
    best = jnp.max(masked[0], axis=0, keepdims=True)
    for e in range(1, own):
        best = jnp.maximum(best, jnp.max(masked[e], axis=0, keepdims=True))
    raised = [jnp.where(ours, jnp.exp(lines - best), 0.0) for lines in masked]
    norm = sum(jnp.sum(lines, axis=0, keepdims=True) for lines in raised)
    for e in range(own):
        share = raised[e] / norm
        combine[e * half:(e + 1) * half] = share
        begin_sum(plain(share.astype(LOW), cot[...]), (0, 1, e))

    tables = {}

    def read_stats(e):
        all_tensor(*stats_of[e]).wait_recv()
        mine = stats[e]
        stats_in[e, me_t] = mine
        most = stats_in[e, 0, 0:1]
        for s in range(1, tp):
            most = jnp.maximum(most, stats_in[e, s, 0:1])
        shrinks = [jnp.exp(stats_in[e, s, 0:1] - most) for s in range(tp)]
        total = sum(stats_in[e, s, 1:2] * shrinks[s] for s in range(tp))
        total_low = sum(stats_in[e, s, 2:3] * shrinks[s] for s in range(tp))
        lines = [
            jnp.exp((stats_in[e, before(k), 0:1] if k else mine[0:1]) - most) / total_low
            for k in range(tp)
        ]
        lines.append(jnp.exp(mine[0:1] - most) / total)
        line_row = iotas((LANES, half))[0]
        table = jnp.zeros((LANES, half), WIDE)
        for s, line in enumerate(lines):
            table = jnp.where(line_row == s, line, table)
        tables[e] = jnp.transpose(table)
        here = slice(e * half, (e + 1) * half)
        dispatch[here] = weight[here] * tables[e][:, tp:tp + 1]

    def pass_on(lot):
        k, e = number[lot], lot[2]
        if lot[0] == 0:
            all_tensor(*tensor_of[k]).wait_recv()
            total_rows = None
            for back in range(tp):
                if back:
                    term = out_recv[k, before(back)]
                else:
                    term = out_send[k, me_t]
                term = term.astype(WIDE).reshape(half, LANES)
                if lot[1] == 0:
                    term = term * tables[e][:, back:back + 1]
                total_rows = term if total_rows is None else total_rows + term
            if lot[1] == 0:
                slot_slice[e * half:(e + 1) * half] = total_rows
            send_slots[k] = total_rows.reshape(depth, PLANE, images, LANES).astype(LOW)
        else:
            all_plane(k, back_recv.at[k - ways]).wait_recv()
            back_recv[k - ways, me_p] = back_send[k - ways, me_p]
            for q in range(PLANE):
                total_rows = back_recv[k - ways, q * tp].astype(WIDE)
                for t in range(1, tp):
                    total_rows = total_rows + back_recv[k - ways, q * tp + t].astype(WIDE)
                send_slots[k, :, q] = total_rows.astype(LOW)
        start_z(*z_of[k])

    def gather(lot, between=None):
        k = number[lot]
        all_z(*z_of[k]).wait_recv()
        if lot[0] == 0:
            slots_out[k, :, me_z] = send_slots[k, me_z]
            start_plane(*plane_of[k])
        else:
            slots_back[k - ways, me_z] = send_slots[k, me_z]
            if between is not None:
                between()
            start_tensor(*tensor_of[k])

    def assembled(lot):
        k, (turn, kind, e) = number[lot], lot
        if turn == 0:
            all_plane(k, full_out.at[k]).wait_recv()
            full_out[k, me_p] = slots_out[k, me_q]
            for q in range(PLANE):
                rows = slice(e * half + q * across, e * half + (q + 1) * across)
                for t in range(tp):
                    block = full_out[k, q * tp + t].astype(WIDE).reshape(across, LANES)
                    flat[turn, kind, rows, t * LANES:(t + 1) * LANES] = block.astype(LOW)
        else:
            all_tensor(*tensor_of[k]).wait_recv()
            full_back[k - ways, me_t] = slots_back[k - ways]
            for t in range(tp):
                block = full_back[k - ways, t].astype(WIDE).reshape(half, LANES)
                flat[turn, kind, e * half:(e + 1) * half, t * LANES:(t + 1) * LANES] = (
                    block.astype(LOW)
                )
        return flat[turn, kind, e * half:(e + 1) * half]

    root = math.sqrt(2.0 / math.pi)
    slope = {}

    def expert_out(e):
        pre = plain(assembled((0, 0, e)), w_in[e])
        square = pre * pre
        bent = jnp.tanh(root * (pre + 0.044715 * (square * pre)))
        hidden[e] = (0.5 * pre * (1.0 + bent)).astype(LOW)
        slope[e] = 0.5 * (1.0 + bent) + 0.5 * pre * (1.0 - bent * bent) * (
            root * (1.0 + 3.0 * 0.044715 * square)
        )
        begin_sum(plain(hidden[e], w_out[e]), (1, 0, e))

    def expert_back(e):
        grad_hidden = rows_by_rows(assembled((0, 1, e)), w_out[e])
        grad_pre[e] = (slope[e] * grad_hidden).astype(LOW)
        begin_sum(rows_by_rows(grad_pre[e], w_in[e]), (1, 1, e))

    read_stats(0)
    pass_on((0, 0, 0))
    read_stats(1)
    pass_on((0, 0, 1))
    pass_on((0, 1, 0))
    gather((0, 0, 0))
    pass_on((0, 1, 1))
    gather((0, 0, 1))
    gather((0, 1, 0))
    for load in loads[3:]:
        load.wait()
    gather((0, 1, 1))
    expert_out(0)
    expert_out(1)
    expert_back(0)
    expert_back(1)
    pass_on((1, 0, 0))
    pass_on((1, 0, 1))
    gather((1, 0, 0))
    pass_on((1, 1, 0))
    gather((1, 0, 1))
    pass_on((1, 1, 1))
    gather((1, 1, 0))

    def send_dots():
        products = jnp.concatenate([
            slots_back[number[(1, 1, e)] - ways].astype(WIDE).reshape(half, LANES)
            for e in range(own)
        ]) * slot_slice[...]
        own_dots = jnp.broadcast_to(jnp.sum(products, axis=1, keepdims=True), (c, LANES))
        dots[...] = jnp.transpose(own_dots)[0:8, :]
        start_tensor(*dots_of)

    gather((1, 1, 1), send_dots)
    for e in range(own):
        here = slice(e * half, (e + 1) * half)
        grad_out[e] = columns_by_columns(hidden[e], flat[0, 1, here]).astype(LOW)
        grad_in[e] = columns_by_columns(flat[0, 0, here], grad_pre[e]).astype(LOW)

    share = combine[...]
    grad_share = jnp.concatenate(
        [rows_by_rows(assembled((1, 0, e)), cot[...]) for e in range(own)]
    )
    row_dot = jnp.sum(grad_share * share, axis=0, keepdims=True)
    from_share = share * (grad_share - row_dot)
    all_tensor(*dots_of).wait_recv()
    dots_in[me_t] = dots[...]
    dot_line = dots_in[0, 0:1]
    for s in range(1, tp):
        dot_line = dot_line + dots_in[s, 0:1]
    column_dot = jnp.transpose(jnp.broadcast_to(dot_line, (LANES, c)))[:, 0:1]
    spots = dispatch[...]
    row, col = iotas((dp, half))
    fold = jnp.where((col >= row * images) & (col < row * images + images), 1.0, 0.0).astype(LOW)
    high = slots // PLANE
    per = PLANE // own
    grad_logits = []

    def start_part(e):
        for jt in sorted(range(tp), key=lambda jt: -min(jt, tp - jt)):
            t = lax.rem(me_t + jt, tp)
            for q in range(e * per, (e + 1) * per):
                copy = remote(
                    part.at[q * tp + t], part_in.at[me_p], p_send.at[sent(PART)], p_recv.at[PART],
                    {"dp": me_z * PLANE + q, "tensor": t},
                )
                if jt:
                    copy.start()
                else:
                    pl.when(me_q != q)(copy.start)

    for e in range(own):
        rows = slice(e * half, (e + 1) * half)
        grad_weight = rows_by_rows(assembled((1, 1, e)), tok[...])
        grad_logits.append(
            (from_share[rows] + spots[rows] * (grad_weight - column_dot[rows])).astype(LOW)
        )
        by_slot = plain(fold, grad_logits[e]).astype(LOW)
        local_router = plain(by_slot, tok[...])
        for q in range(per):
            for t in range(tp):
                part[(e * per + q) * tp + t] = local_router[
                    q * high:(q + 1) * high, t * LANES:(t + 1) * LANES
                ].astype(LOW)
        start_part(e)
    grad_logits = jnp.concatenate(grad_logits)
    slot_grad = flat[1, 1]
    grad_tok[...] = (
        columns_by_columns(spots.astype(LOW), slot_grad)
        + columns_by_columns(grad_logits, spread[...])
    ).astype(LOW)

    all_plane(PART, part_in).wait_recv()
    part_in[me_p] = part[me_p]
    piece[...] = jnp.sum(part_in[...].astype(WIDE), axis=0)
    piece_of = (PIECE, lambda to: piece, piece_in.at[me_z], piece_in.at[few_z])
    start_z(*piece_of)
    all_z(*piece_of).wait_recv()
    piece_in[me_z] = piece[...]
    final[...] = jnp.sum(piece_in[...], axis=0).astype(LOW)
    start_plane(WHOLE, lambda q, t: final, whole.at[me_p])
    all_plane(WHOLE, whole).wait_recv()
    whole[me_p] = final[...]
    row, col = iotas((slots, slots))
    order = jnp.where(col == lax.rem(row, own) * dp + row // own, 1.0, 0.0).astype(LOW)
    for t in range(tp):
        lines = jnp.concatenate([whole[q * tp + t] for q in range(PLANE)])
        grad_router[:, t * LANES:(t + 1) * LANES] = plain(order, lines)

    few_p = pl.ds(0, members - 1)
    waits = [
        (t_send.at[0], out_recv.at[:, few_t]), (t_send.at[1], full_back.at[:, few_t]),
        (t_send.at[2], dots_in.at[few_t]), (t_send.at[3], stats_in.at[:, few_t]),
        (p_send.at[0], full_out.at[:, few_p]), (p_send.at[1], back_recv.at[:, few_p]),
        (p_send.at[2], part_in.at[few_p]), (p_send.at[3], whole.at[few_p]),
        (z_send.at[0], send_slots.at[:, few_z]), (z_send.at[1], piece_in.at[few_z]),
    ]
    for sem, bulk in waits:
        remote(bulk, bulk, sem, t_recv.at[0], {"tensor": lax.rem(me_t + 1, tp)}).wait_send()


def finish(*refs):
    count = (len(refs) - 1) // 2
    copies = [
        pltpu.make_async_copy(refs[k], refs[count + k], refs[-1].at[k]) for k in range(count)
    ]
    for copy in copies:
        copy.start()
    for copy in copies:
        copy.wait()


def on_device(tokens, cotangent, dispatch_weight, w_in, w_out):
    tp, dp = lax.axis_size("tensor"), lax.axis_size("dp")
    images, seq, width = tokens.shape
    own, _, inner = w_in.shape
    n, slots, group = images * seq, dp * own, own * images
    c = dp * group
    members, depth, high, ways = PLANE * tp, dp // PLANE, slots // PLANE, 2 * own
    vmem, hbm = pltpu.VMEM, pl.BlockSpec(memory_space=pltpu.HBM)
    here = pl.BlockSpec(memory_space=pltpu.VMEM)
    shapes = [((n, width), LOW), ((slots, width), WIDE), (w_in.shape, LOW), (w_out.shape, LOW)]
    outs = pl.pallas_call(
        functools.partial(kernel, tp, dp, images, own),
        name="moe_back",
        out_shape=tuple(vmem(*shape) for shape in shapes),
        in_specs=[hbm] * 5,
        out_specs=(here,) * 4,
        scratch_shapes=[
            vmem((slots, width), LOW), vmem((n, width), LOW), vmem((n, width), LOW),
            vmem(w_in.shape, LOW), vmem(w_out.shape, LOW),
            vmem((c, width), LOW),
            vmem((c, n), WIDE), vmem((c, n), WIDE), vmem((c, n), WIDE),
            vmem((c, LANES), WIDE),
            vmem((ways, tp, dp, images, LANES), LOW), vmem((ways, tp, dp, images, LANES), LOW),
            vmem((ways, members, depth, images, LANES), LOW),
            vmem((ways, members, depth, images, LANES), LOW),
            vmem((2 * ways, depth, PLANE, images, LANES), LOW),
            vmem((ways, PLANE, depth, images, LANES), LOW),
            vmem((ways, depth, PLANE, images, LANES), LOW),
            vmem((ways, members, depth, images, LANES), LOW),
            vmem((ways, tp, depth, PLANE, images, LANES), LOW),
            vmem((2, 2, c, width), LOW),
            vmem((own, c // own, inner), LOW), vmem((own, c // own, inner), LOW),
            vmem((own, 8, c // own), WIDE), vmem((own, tp, 8, c // own), WIDE),
            vmem((8, c), WIDE), vmem((tp, 8, c), WIDE),
            vmem((members, high, LANES), LOW), vmem((members, high, LANES), LOW),
            vmem((high, LANES), WIDE), vmem((depth, high, LANES), WIDE),
            vmem((members, high, LANES), LOW), vmem((high, LANES), LOW),
            pltpu.SemaphoreType.DMA((5,)),
            pltpu.SemaphoreType.DMA((4,)), pltpu.SemaphoreType.DMA((2 * ways + 1 + own,)),
            pltpu.SemaphoreType.DMA((4,)), pltpu.SemaphoreType.DMA((2 * ways + 2,)),
            pltpu.SemaphoreType.DMA((2,)), pltpu.SemaphoreType.DMA((2 * ways + 1,)),
        ],
        compiler_params=pltpu.CompilerParams(
            collective_id=0, has_side_effects=True, vmem_limit_bytes=61400000
        ),
    )(
        dispatch_weight.T, tokens.reshape(n, width), cotangent.reshape(n, width), w_in, w_out
    )
    grad_tokens, grad_router, grad_w_in, grad_w_out = pl.pallas_call(
        finish,
        name="finish",
        out_shape=tuple(jax.ShapeDtypeStruct(*shape) for shape in shapes),
        in_specs=[here] * 4,
        out_specs=(hbm,) * 4,
        scratch_shapes=[pltpu.SemaphoreType.DMA((4,))],
        compiler_params=pltpu.CompilerParams(vmem_limit_bytes=4 * 2**20),
    )(*outs)
    return (grad_tokens.reshape(tokens.shape), grad_router.T, grad_w_in, grad_w_out)


def solution(mesh):
    return jax.shard_map(
        on_device,
        mesh=mesh,
        in_specs=(
            P("dp", "tensor", None),
            P("dp", "tensor", None),
            P(),
            P("dp", None, "tensor"),
            P("dp", "tensor", None),
        ),
        out_specs=(P("dp", "tensor", None), P(), P("dp", None, "tensor"), P("dp", "tensor", None)),
        check_vma=False,
    )
```
